8 devices in a mesh: dp: 2 (over y, z), tp: 4 (over x, core).
Axes of the slice: x: 2, y: 2, z: 1, core: 2. Of those that a mesh axis runs over, the one named last changes fastest.
Arguments:
- x: bfloat16 [8, 512, 4096], P('dp'), parts along dimension 0
- gain_a: bfloat16 [4096], replicated
- wq: bfloat16 [4096, 4096], P(None, 'tp')
- wk: bfloat16 [4096, 1024], P(None, 'tp')
- wv: bfloat16 [4096, 1024], P(None, 'tp')
- wo: bfloat16 [4096, 4096], P('tp')
- gain_m: bfloat16 [4096], replicated
- w_gate: bfloat16 [4096, 12800], P(None, 'tp')
- w_up: bfloat16 [4096, 12800], P(None, 'tp')
- w_down: bfloat16 [12800, 4096], P('tp')
Outputs:
- output: bfloat16 [8, 512, 4096], P('dp'), parts along dimension 0
There are 2 independent parts. The reference program is written for one: setup_inputs(seed, part) draws one part's arguments, and reference() takes and returns one part's arrays. A program takes and returns all parts, laid end to end along the dimension named above; an argument that names none is the same for every part.
All inputs are finite; a program needn't handle non-finite values.
Results may differ from the reference program's by a relative error of at most 0.017.
Values are sent between devices in bfloat16 or wider.
A program may use at most 2 GiB of HBM per device.

```python
import jax
import jax.numpy as jnp
from jax import lax

SEQUENCES = 4
TOKENS = 512
D = 4096
HEADS = 32
KV_HEADS = 8
HEAD = 128
FF = 12800
THETA = 10000


def setup_inputs(seed: int = 0, part: int = 0) -> dict:
    kx, ka, km, kq, kk, kv, ko, kg, ku, kd = jax.random.split(jax.random.key(seed), 10)

    def weights(key, rows, columns):
        return jax.random.normal(key, (rows, columns), jnp.float32) * rows**-0.5

    drawn = {
        "x": jax.random.normal(jax.random.fold_in(kx, part), (SEQUENCES, TOKENS, D), jnp.float32),
        "gain_a": 1 + 0.1 * jax.random.normal(ka, (D,), jnp.float32),
        "wq": 2 * weights(kq, D, HEADS * HEAD),
        "wk": 2 * weights(kk, D, KV_HEADS * HEAD),
        "wv": 4 * weights(kv, D, KV_HEADS * HEAD),
        "wo": weights(ko, HEADS * HEAD, D),
        "gain_m": 1 + 0.1 * jax.random.normal(km, (D,), jnp.float32),
        "w_gate": weights(kg, D, FF),
        "w_up": weights(ku, D, FF),
        "w_down": 3 * weights(kd, FF, D),
    }
    return {k: v.astype(jnp.bfloat16) for k, v in drawn.items()}


def normed(x, gain):
    wide = x.astype(jnp.float32)
    scale = lax.rsqrt(jnp.mean(wide * wide, -1, keepdims=True) + 1e-6)
    return (wide * scale * gain.astype(jnp.float32)).astype(jnp.bfloat16)


def turned(t, place, theta):
    half = t.shape[-1] // 2
    angle = place.astype(jnp.float32)[:, None] * theta ** (-jnp.arange(half, dtype=jnp.float32) / half)
    cos, sin = jnp.cos(angle)[:, None], jnp.sin(angle)[:, None]
    a, b = t[..., :half].astype(jnp.float32), t[..., half:].astype(jnp.float32)
    return jnp.concatenate([a * cos - b * sin, b * cos + a * sin], -1).astype(jnp.bfloat16)


def matmul(a, w):
    return jnp.dot(a, w, preferred_element_type=jnp.float32).astype(jnp.bfloat16)


def einsum(form, a, b):
    return jnp.einsum(form, a.astype(jnp.float32), b.astype(jnp.float32))


def attention(q, k, v):
    scores = einsum("tgsd,ugd->gstu", q, k) * q.shape[-1] ** -0.5
    token = jnp.arange(q.shape[0])
    scores = jnp.where(token[:, None] >= token, scores, -jnp.inf)
    weights = jax.nn.softmax(scores, -1).astype(jnp.bfloat16)
    return einsum("gstu,ugd->tgsd", weights, v).astype(jnp.bfloat16)


def one(x, gain_a, wq, wk, wv, wo, gain_m, w_gate, w_up, w_down):
    rows = x.shape[0]
    a, place = normed(x, gain_a), jnp.arange(rows)
    k = turned(matmul(a, wk).reshape(rows, -1, HEAD), place, THETA)
    q = turned(matmul(a, wq).reshape(rows, -1, HEAD), place, THETA).reshape(rows, k.shape[1], -1, HEAD)
    v = matmul(a, wv).reshape(rows, -1, HEAD)
    seen = attention(q, k, v).reshape(rows, -1)
    h = (x.astype(jnp.float32) + jnp.dot(seen, wo, preferred_element_type=jnp.float32)).astype(jnp.bfloat16)
    b = normed(h, gain_m)
    gate = jnp.dot(b, w_gate, preferred_element_type=jnp.float32)
    up = jnp.dot(b, w_up, preferred_element_type=jnp.float32)
    hidden = (jax.nn.silu(gate) * up).astype(jnp.bfloat16)
    return (h.astype(jnp.float32) + jnp.dot(hidden, w_down, preferred_element_type=jnp.float32)).astype(jnp.bfloat16)


def reference(x, gain_a, wq, wk, wv, wo, gain_m, w_gate, w_up, w_down):
    return lax.map(lambda sequence: one(sequence, gain_a, wq, wk, wv, wo, gain_m, w_gate, w_up, w_down), x)
```

```python
import functools

import jax
import jax.numpy as jnp
from jax import lax
from jax.experimental import pallas as pl
from jax.experimental.pallas import tpu as pltpu
from jax.sharding import PartitionSpec as P

HEAD = 128
THETA = 10000
LOG2E = 1.4426950408889634
SAME_CHIP = [(0, 1), (1, 0), (2, 3), (3, 2)]
OTHER_CHIP = [(0, 2), (2, 0), (1, 3), (3, 1)]
PIECE = 512
VMEM = 63 * 2**20


def _dot(a, b, ca=1, cb=0):
    return lax.dot_general(a, b, (((ca,), (cb,)), ((), ())), preferred_element_type=jnp.float32)


def rotary(rows):
    half = HEAD // 2
    angle = jnp.arange(rows, dtype=jnp.float32)[:, None] * THETA ** (-jnp.arange(half, dtype=jnp.float32) / half)
    cos, sin = jnp.cos(angle), jnp.sin(angle)
    return jnp.concatenate([cos, cos], -1), jnp.concatenate([-sin, sin], -1)


def _turned(t, cos, sin):
    t = t.astype(jnp.float32)
    return (t * cos + pltpu.roll(t, HEAD // 2, 1) * sin).astype(jnp.bfloat16)


def _normed(parts, gains):
    wide = [p.astype(jnp.float32) for p in parts]
    total = sum(jnp.sum(w * w, -1, keepdims=True) for w in wide)
    scale = lax.rsqrt(total * (1 / sum(w.shape[1] for w in wide)) + 1e-6)
    return [(w * scale * g).astype(jnp.bfloat16) for w, g in zip(wide, gains)]


def _places():
    me = lax.axis_index("tp")
    core = lax.rem(me, 2)
    return core, me + 1 - 2 * core


def _greet(peer):
    pl.semaphore_signal(pltpu.get_barrier_semaphore(), inc=1, device_id={"tp": peer}, device_id_type=pl.DeviceIdType.MESH)


def _to_core(peer, src, dst, send, recv):
    return pltpu.make_async_remote_copy(
        src_ref=src, dst_ref=dst, send_sem=send, recv_sem=recv, device_id={"tp": peer}, device_id_type=pl.DeviceIdType.MESH
    )


def _sum_on_chip(peer, term, n, out_ref, send_s, recv_s, sum_s, send_sem, recv_sem, out_sem):
    def over(i):
        return _to_core(peer, send_s.at[i], recv_s.at[i], send_sem.at[i], recv_sem.at[i])

    def out(i):
        return pltpu.make_async_copy(sum_s.at[i], out_ref.at[:, pl.ds(pl.multiple_of(i * PIECE, PIECE), PIECE)], out_sem.at[i])

    def away(i, _):
        send_s[i] = term(i).astype(jnp.bfloat16)
        over(i).start()

    def here(i, _):
        t = term(n + i)
        over(i).wait_recv()
        sum_s[i] = (t + recv_s[i].astype(jnp.float32)).astype(jnp.bfloat16)
        out(i).start()

    def done(i, _):
        over(i).wait_send()
        out(i).wait()

    for step in (away, here, done):
        lax.fori_loop(0, n, step, None)


def _first(x_ref, gain_ref, cos_ref, sin_ref, wq_ref, wk_ref, wv_ref, wo_ref, out_ref,
           x_s, a_s, w_s, wo_s, qkv_s, seen_s, send_s, recv_s, sum_s, x_sem, w_sem, wo_sem, send_sem, recv_sem, out_sem, *, first):
    rows, d = x_s.shape
    width = w_s.shape[2]
    n = d // 2 // PIECE
    core, peer = _places()
    _greet(peer)

    load = rows // 4
    loads = [pltpu.make_async_copy(x_ref.at[pl.ds(first + i * load, load), :], x_s.at[pl.ds(i * load, load), :], x_sem.at[i]) for i in range(4)]
    pieces = [wk_ref, wv_ref, *(wq_ref.at[:, pl.ds(i * width, width)] for i in range(w_s.shape[0] - 2))]
    weights = [pltpu.make_async_copy(w, w_s.at[i], w_sem.at[i]) for i, w in enumerate(pieces)]

    def wo_copy(i):
        half = jnp.where(i < n, 1 - core, core)
        at = pl.multiple_of(half * (d // 2) + lax.rem(i, n) * PIECE, PIECE)
        return pltpu.make_async_copy(wo_ref.at[:, pl.ds(at, PIECE)], wo_s.at[i], wo_sem.at[i])

    for c in (*loads, *weights):
        c.start()
    for i in range(2 * n):
        wo_copy(i).start()

    step = 32
    gain = gain_ref[...].astype(jnp.float32)
    for i in range(4):
        loads[i].wait()

        def norm(j, _):
            here = pl.ds(pl.multiple_of(i * load + j * step, step), step)
            a_s[here, :] = _normed([x_s[here, :]], [gain])[0]

        lax.fori_loop(0, load // step, norm, None)

    def project(i, _):
        pltpu.make_async_copy(wk_ref, w_s.at[i], w_sem.at[i]).wait()
        qkv_s[i] = _dot(a_s[...], w_s[i]).astype(jnp.bfloat16)

    lax.fori_loop(0, w_s.shape[0], project, None)

    block = 256
    e = HEAD**-0.5 * LOG2E

    def attend(g, _):
        column = pl.ds(pl.multiple_of(g * HEAD, HEAD), HEAD)
        k = _turned(qkv_s[0, :, column], cos_ref[...], sin_ref[...])
        values = jnp.concatenate([qkv_s[1, :, column].T, jnp.ones((8, rows), jnp.bfloat16)], axis=0)
        hidden = lax.broadcasted_iota(jnp.int32, (block, block), 0) > lax.broadcasted_iota(jnp.int32, (block, block), 1)
        for at in range(0, rows, block):
            here, keys = slice(at, at + block), at + block
            cos, sin = cos_ref[here, :], sin_ref[here, :]
            scores = []
            for h in range(4):
                q = qkv_s[2 + 2 * g + h // 2, here, h % 2 * HEAD : (h % 2 + 1) * HEAD]
                scores.append(_dot(k[:keys], _turned(q, cos, sin), 1, 1))
            weights = []
            for s in scores:
                last = jnp.where(hidden, -1e30, s[at:])
                s = jnp.concatenate([s[:at], last], axis=0) if at else last
                weights.append(jnp.exp2((s - s.max(axis=0, keepdims=True)) * e).astype(jnp.bfloat16))
            for h, p in enumerate(weights):
                mix = _dot(values[:, :keys], p)
                out = (mix[:HEAD] * (1 / mix[HEAD : HEAD + 1])).T.astype(jnp.bfloat16)
                seen_s[here, pl.ds(pl.multiple_of((g * 4 + h) * HEAD, HEAD), HEAD)] = out

    lax.fori_loop(0, 2, attend, None)

    def term(i):
        wo_copy(i).wait()
        return _dot(seen_s[...], wo_s[i])

    pl.semaphore_wait(pltpu.get_barrier_semaphore(), 1)
    _sum_on_chip(peer, term, n, out_ref, send_s, recv_s, sum_s, send_sem, recv_sem, out_sem)


def _second(x_ref, chip_ref, other_ref, gain_ref, wg_ref, wu_ref, wd_ref, after_ref, out_ref, mine_ref,
            in_s, h_s, b_s, g_s, u_s, hidden_s, wd_s, send_s, recv_s, sum_s,
            in_sem, h_out_sem, h_send_sem, h_recv_sem, w_sem, wd_sem, send_sem, recv_sem, out_sem, *, first):
    rows, d = b_s.shape
    half, wide = d // 2, g_s.shape[2]
    blocks, slots = wg_ref.shape[1] // wide, wd_s.shape[0]
    n = half // PIECE
    core, peer = _places()
    _greet(peer)

    def weight_copies(i):
        at = pl.ds(pl.multiple_of(i * wide, HEAD), wide)
        slot = lax.rem(i, 2)
        return [pltpu.make_async_copy(w.at[:, at], s.at[slot], w_sem.at[m, slot]) for m, (w, s) in enumerate(((wg_ref, g_s), (wu_ref, u_s)))]

    def down_copy(i):
        side = jnp.where(i < n, 1 - core, core)
        at = pl.multiple_of(side * half + lax.rem(i, n) * PIECE, PIECE)
        slot = lax.rem(i, slots)
        return pltpu.make_async_copy(wd_ref.at[:, pl.ds(at, PIECE)], wd_s.at[slot], wd_sem.at[slot])

    load = rows // 4
    columns = pl.ds(pl.multiple_of(core * half, half), half)

    def inputs(i):
        here = pl.ds(i * load, load)
        given = (x_ref.at[pl.ds(first + i * load, load), columns], chip_ref.at[here, :], other_ref.at[here, :])
        return [pltpu.make_async_copy(r, in_s.at[m, here, :], in_sem.at[m, i]) for m, r in enumerate(given)]

    def h_over(i):
        here = h_s.at[core, pl.ds(i * load, load), :]
        return _to_core(peer, here, here, h_send_sem.at[i], h_recv_sem.at[i])

    for i in range(4):
        for c in inputs(i):
            c.start()
    for i in range(2):
        for c in weight_copies(i):
            c.start()

    step = 32
    pl.semaphore_wait(pltpu.get_barrier_semaphore(), 1)
    for i in range(4):
        for c in inputs(i):
            c.wait()

        def add(j, _):
            here = pl.ds(pl.multiple_of(i * load + j * step, step), step)
            x, a, b = (in_s[m, here, :].astype(jnp.float32) for m in range(3))
            h_s[core, here, :] = (x + (a + b)).astype(jnp.bfloat16)

        lax.fori_loop(0, load // step, add, None)
        h_over(i).start()
    kept = pltpu.make_async_copy(h_s.at[core], mine_ref, h_out_sem)
    kept.start()
    for i in range(slots):
        down_copy(i).start()

    gains = [gain_ref[:, :half].astype(jnp.float32), gain_ref[:, half:].astype(jnp.float32)]
    for i in range(4):
        h_over(i).wait_recv()

        def norm(j, _):
            here = pl.ds(pl.multiple_of(i * load + j * step, step), step)
            b_s[here, :half], b_s[here, half:] = _normed([h_s[0, here, :], h_s[1, here, :]], gains)

        lax.fori_loop(0, load // step, norm, None)

    def block(i, _):
        slot = lax.rem(i, 2)
        for c in weight_copies(i):
            c.wait()

        def part(j, _):
            at = pl.ds(pl.multiple_of(j * HEAD, HEAD), HEAD)
            both = _dot(b_s[...], jnp.concatenate([g_s[slot, :, at], u_s[slot, :, at]], axis=1))
            hidden_s[:, pl.ds(pl.multiple_of(i * wide + j * HEAD, HEAD), HEAD)] = (jax.nn.silu(both[:, :HEAD]) * both[:, HEAD:]).astype(jnp.bfloat16)

        lax.fori_loop(0, wide // HEAD, part, None)

        @pl.when(i + 2 < blocks)
        def _():
            for c in weight_copies(i + 2):
                c.start()

    lax.fori_loop(0, blocks, block, None)

    def term(i):
        down_copy(i).wait()
        t = _dot(hidden_s[...], wd_s[lax.rem(i, slots)])

        @pl.when(i + slots < 2 * n)
        def _():
            down_copy(i + slots).start()

        return t

    _sum_on_chip(peer, term, n, out_ref, send_s, recv_s, sum_s, send_sem, recv_sem, out_sem)
    for i in range(4):
        h_over(i).wait_send()
    kept.wait()


def solution(mesh):
    def step(x, gain_a, wq, wk, wv, wo, gain_m, w_gate, w_up, w_down):
        batch, rows, d = x.shape
        half, n, low = d // 2, d // 2 // PIECE, jnp.bfloat16
        core = lax.rem(lax.axis_index("tp"), 2)
        cos, sin = rotary(rows)
        x2 = x.reshape(batch * rows, d)
        dma, anywhere, inside = pltpu.SemaphoreType.DMA, pl.BlockSpec(memory_space=pl.ANY), pl.BlockSpec(memory_space=pltpu.VMEM)
        exchange = [pltpu.VMEM((n, rows, PIECE), low)] * 3
        exchange_sems = [dma((n,))] * 3

        def first_half(s):
            pieces = wq.shape[1] // (2 * HEAD) + 2
            return pl.pallas_call(
                functools.partial(_first, first=s * rows),
                in_specs=[anywhere, inside, inside, inside, *[anywhere] * 4],
                out_specs=anywhere,
                out_shape=jax.ShapeDtypeStruct((rows, half), low),
                scratch_shapes=[
                    pltpu.VMEM((rows, d), low), pltpu.VMEM((rows, d), low), pltpu.VMEM((pieces, d, 2 * HEAD), low),
                    pltpu.VMEM((2 * n, wo.shape[0], PIECE), low), pltpu.VMEM((pieces, rows, 2 * HEAD), low), pltpu.VMEM((rows, wo.shape[0]), low),
                    *exchange, dma((4,)), dma((pieces,)), dma((2 * n,)), *exchange_sems,
                ],
                compiler_params=pltpu.CompilerParams(collective_id=s, has_side_effects=True, vmem_limit_bytes=VMEM),
                cost_estimate=pl.CostEstimate(flops=2 * rows * d * (2560 + 256), transcendentals=8 * rows * rows, bytes_accessed=26 * 2**20),
                name=f"first_{s}",
            )(x2, gain_a.reshape(1, d), cos, sin, wq, wk, wv, wo)

        def second_half(s, chip, other, after):
            wide, slots = 640, 3
            return pl.pallas_call(
                functools.partial(_second, first=s * rows),
                in_specs=[anywhere, anywhere, anywhere, inside, *[anywhere] * 4],
                out_specs=[anywhere, anywhere],
                out_shape=[jax.ShapeDtypeStruct((rows, half), low)] * 2,
                scratch_shapes=[
                    pltpu.VMEM((3, rows, half), low), pltpu.VMEM((2, rows, half), low), pltpu.VMEM((rows, d), low),
                    pltpu.VMEM((2, d, wide), low), pltpu.VMEM((2, d, wide), low), pltpu.VMEM((rows, w_down.shape[0]), low),
                    pltpu.VMEM((slots, w_down.shape[0], PIECE), low), *exchange,
                    dma((3, 4)), dma, dma((4,)), dma((4,)), dma((2, 2)), dma((slots,)), *exchange_sems,
                ],
                compiler_params=pltpu.CompilerParams(collective_id=batch + s, has_side_effects=True, vmem_limit_bytes=VMEM),
                cost_estimate=pl.CostEstimate(flops=6 * rows * d * w_down.shape[0], transcendentals=rows * w_down.shape[0], bytes_accessed=84 * 2**20),
                name=f"second_{s}",
            )(x2, chip, other, gain_m.reshape(1, d), w_gate, w_up, w_down, after)

        chips = [first_half(s) for s in range(batch)]
        others = [lax.ppermute(t, "tp", OTHER_CHIP) for t in chips]
        after, ends = chips[-1], []
        for s in range(batch):
            chip, mine = second_half(s, chips[s], others[s], after)
            after = chip
            ends.append((mine, chip, lax.ppermute(chip, "tp", OTHER_CHIP)))
        ys = []
        for mine, chip, other in ends:
            y = (mine.astype(jnp.float32) + (chip.astype(jnp.float32) + other.astype(jnp.float32))).astype(low)
            second = lax.ppermute(y, "tp", SAME_CHIP)
            ys.append(jnp.where(core == 0, jnp.concatenate([y, second], 1), jnp.concatenate([second, y], 1)))
        return jnp.stack(ys)

    tokens, whole, columns, rows_of = P("dp", None, None), P(None), P(None, "tp"), P("tp", None)
    return jax.shard_map(
        step,
        mesh=mesh,
        in_specs=(tokens, whole, columns, columns, columns, rows_of, whole, columns, columns, rows_of),
        out_specs=tokens,
        check_vma=False,
    )
```

```python
import functools

import jax
import jax.numpy as jnp
import numpy as np
from jax import lax
from jax.experimental import pallas as pl
from jax.experimental.pallas import tpu as pltpu
from jax.sharding import PartitionSpec as P


HEAD = 128
THETA = 10000
LOG2E = 1.4426950408889634
SAME_CHIP = [(0, 1), (1, 0), (2, 3), (3, 2)]
OTHER_CHIP = [(0, 2), (2, 0), (1, 3), (3, 1)]
FINE = 16
GROUPS = (4, 2, 2)
CHUNK = 256
PIECE = 1024
VMEM = 63 * 2**20


def _dot(a, b, ca=1, cb=0):
    return lax.dot_general(a, b, (((ca,), (cb,)), ((), ())), preferred_element_type=jnp.float32)


def rotary(rows):
    half = HEAD // 2
    place = np.concatenate([np.arange(0, rows, FINE), np.arange(FINE)])
    angle = place[:, None] * float(THETA) ** (-np.arange(half) / half)
    return np.stack([np.tile(f(angle), 2) for f in (np.cos, np.sin)]).astype(np.float32)


def _turned(t, cos, sin):
    t = t.astype(jnp.float32)
    return (t * cos + pltpu.roll(t, HEAD // 2, 1) * sin).astype(jnp.bfloat16)


def _normed(parts, gains):
    wide = [p.astype(jnp.float32) for p in parts]
    total = sum(jnp.sum(w * w, -1, keepdims=True) for w in wide)
    scale = lax.rsqrt(total * (1 / sum(w.shape[1] for w in wide)) + 1e-6)
    return [(w * scale * g).astype(jnp.bfloat16) for w, g in zip(wide, gains)]


def _places():
    me = lax.axis_index("tp")
    core = lax.rem(me, 2)
    return core, me + 1 - 2 * core


def _greet(peer):
    pl.semaphore_signal(pltpu.get_barrier_semaphore(), inc=1, device_id={"tp": peer}, device_id_type=pl.DeviceIdType.MESH)


def _to_core(peer, src, dst, send, recv):
    return pltpu.make_async_remote_copy(
        src_ref=src, dst_ref=dst, send_sem=send, recv_sem=recv, device_id={"tp": peer}, device_id_type=pl.DeviceIdType.MESH
    )


def _sum_on_chip(peer, term, out_refs, send_s, recv_s, own_s, sum_s, send_sem, recv_sem, out_sem):
    n, rows = send_s.shape[0], send_s.shape[1]
    per = n // len(out_refs)

    def over(i):
        return _to_core(peer, send_s.at[i], recv_s.at[i], send_sem.at[i], recv_sem.at[i])

    def out(i):
        return pltpu.make_async_copy(sum_s.at[i], out_refs[i // per].at[:, pl.ds(i % per * PIECE, PIECE)], out_sem.at[i])

    def finish(i):
        over(i).wait_recv()
        sum_s[i] = (own_s[lax.rem(i, 2)] + recv_s[i].astype(jnp.float32)).astype(jnp.bfloat16)

    def piece(i, _):
        t = term(i)
        send_s[i] = t[:rows].astype(jnp.bfloat16)
        own_s[lax.rem(i, 2)] = t[rows:]
        over(i).start()

        @pl.when(i > 0)
        def _():
            finish(i - 1)

    lax.fori_loop(0, n, piece, None)
    for i in range(n - 1):
        out(i).start()
    finish(n - 1)
    out(n - 1).start()
    for i in range(n):
        over(i).wait_send()
        out(i).wait()


def _group(groups, chunk):
    for i, count in enumerate(groups):
        if chunk < count:
            return i, chunk
        chunk -= count


def _first(x_ref, gain_ref, turn_ref, wq_ref, wk_ref, wv_ref, wo_ref, *rest, groups_of, crossing):
    chip_refs, other_ref, rest = rest[: len(groups_of)], rest[len(groups_of)], rest[len(groups_of) + 1 :]
    (x_s, a_s, w_s, wo_s, qkv_s, keys_s, seen_s, turn_s, send_s, recv_s, own_s, sum_s,
     x_sem, w_sem, wo_sem, send_sem, recv_sem, out_sem, x_send_sem, x_recv_sem) = rest
    rows, _ = a_s.shape
    half, width, n, chunks = rows // 2, w_s.shape[2], wo_s.shape[0], sum_s.shape[0] // wo_s.shape[0]
    groups = wk_ref.shape[1] // HEAD
    core, peer = _places()
    across = lax.rem(lax.axis_index("tp") + 2, 4)
    _greet(peer)
    _greet(across)

    weights = [pltpu.make_async_copy(w, w_s.at[0, :, pl.ds(i * width // 2, width // 2)], w_sem.at[i]) for i, w in enumerate((wk_ref, wv_ref))]
    weights += [pltpu.make_async_copy(wq_ref.at[:, pl.ds(i * width, width)], w_s.at[i + 1], w_sem.at[i + 2]) for i in range(w_s.shape[0] - 1)]

    def x_copy(c):
        return pltpu.make_async_copy(x_ref.at[pl.ds(pl.multiple_of(c * rows, rows), rows), :], x_s.at[lax.rem(c, 2)], x_sem.at[lax.rem(c, 2)])

    def wo_copy(i):
        return pltpu.make_async_copy(wo_ref.at[:, pl.ds(pl.multiple_of(i * PIECE, PIECE), PIECE)], wo_s.at[i], wo_sem.at[i])

    x_copy(0).start()
    for c in weights:
        c.start()

    sign = jnp.where(lax.broadcasted_iota(jnp.int32, (1, HEAD), 1) < HEAD // 2, -1.0, 1.0)
    coarse = turn_ref.shape[1] - FINE
    cos, sin = turn_ref[0, coarse:, :], turn_ref[1, coarse:, :]
    for i in range(coarse):
        c, s = turn_ref[0, i : i + 1, :], turn_ref[1, i : i + 1, :]
        turn_s[0, i * FINE : (i + 1) * FINE, :] = cos * c - sin * s
        turn_s[1, i * FINE : (i + 1) * FINE, :] = (sin * c + cos * s) * sign

    gain = gain_ref[...].astype(jnp.float32)
    step = 32
    e = HEAD**-0.5 * LOG2E
    hidden = lax.broadcasted_iota(jnp.int32, (rows, rows), 0) > lax.broadcasted_iota(jnp.int32, (rows, rows), 1)

    def over(c, i):
        slot = lax.rem(c, 2) * n + i
        return _to_core(peer, send_s.at[slot], recv_s.at[slot], send_sem.at[slot], recv_sem.at[slot])

    def cross(i):
        to = other_ref.at[pl.ds(i // n * half, half), pl.ds(i % n * PIECE, PIECE)]
        return _to_core(across, sum_s.at[i], to, x_send_sem.at[i], x_recv_sem.at[i])

    def out(c, i):
        array, first = _group(groups_of, c)
        return pltpu.make_async_copy(
            sum_s.at[c * n + i], chip_refs[array].at[pl.ds(first * half, half), pl.ds(i * PIECE, PIECE)], out_sem.at[c * n + i]
        )

    def chunk(c, _):
        slot, late = lax.rem(c, 2), lax.rem(c, 2)
        place = pl.multiple_of(late * rows, rows)
        x_copy(c).wait()

        @pl.when(c + 1 < chunks)
        def _():
            x_copy(c + 1).start()

        def norm(j, _):
            here = pl.ds(pl.multiple_of(j * step, step), step)
            a_s[here, :] = _normed([x_s[slot, here, :]], [gain])[0]

        lax.fori_loop(0, rows // step, norm, None)

        @pl.when(c == 0)
        def _():
            for i in range(n):
                wo_copy(i).start()
            for w in weights[:2]:
                w.wait()

        def project(i, _):
            @pl.when((i > 0) & (c == 0))
            def _():
                pltpu.make_async_copy(wq_ref.at[:, pl.ds(0, width)], w_s.at[i], w_sem.at[i + 1]).wait()

            qkv_s[i] = _dot(a_s[...], w_s[i]).astype(jnp.bfloat16)

        lax.fori_loop(0, w_s.shape[0], project, None)
        new = pl.ds(place, rows)
        for g in range(groups):
            keys_s[new, g * HEAD : (g + 1) * HEAD] = _turned(qkv_s[0, :, g * HEAD : (g + 1) * HEAD], turn_s[0, new, :], turn_s[1, new, :])
        keys_s[new, groups * HEAD :] = qkv_s[0, :, groups * HEAD :]

        def attend(g, _, before):
            total = before + rows
            k = keys_s[:total, pl.ds(pl.multiple_of(g * HEAD, HEAD), HEAD)]
            v = keys_s[:total, pl.ds(pl.multiple_of((g + groups) * HEAD, HEAD), HEAD)]
            values = jnp.concatenate([v.T, jnp.ones((8, total), jnp.bfloat16)], axis=0)
            scores = []
            for h in range(4):
                q = _turned(qkv_s[1 + g, :, h * HEAD : (h + 1) * HEAD], turn_s[0, before:total, :], turn_s[1, before:total, :])
                scores.append(_dot(k, q, 1, 1))
            found = []
            for s in scores:
                last = jnp.where(hidden, -1e30, s[before:])
                s = jnp.concatenate([s[:before], last], axis=0) if before else last
                found.append(jnp.exp2((s - s.max(axis=0, keepdims=True)) * e).astype(jnp.bfloat16))
            for h, p in enumerate(found):
                mix = _dot(values, p)
                got = (mix[:HEAD] * (1 / mix[HEAD : HEAD + 1])).T.astype(jnp.bfloat16)
                for part in range(2):
                    to = pl.ds(pl.multiple_of(jnp.where(core == part, half, 0), half), half)
                    seen_s[to, pl.ds(pl.multiple_of((g * 4 + h) * HEAD, HEAD), HEAD)] = got[part * half : (part + 1) * half]

        for p in range(2):
            pl.when(late == p)(lambda p=p: lax.fori_loop(0, groups, functools.partial(attend, before=p * rows), None))

        @pl.when(c == 0)
        def _():
            pl.semaphore_wait(pltpu.get_barrier_semaphore(), 2)

        def finish(i):
            over(c, i).wait_recv()
            sum_s[c * n + i] = (own_s[lax.rem(i, 2)] + recv_s[late * n + i].astype(jnp.float32)).astype(jnp.bfloat16)
            for k in range(crossing):
                pl.when(c * n + i == k)(lambda k=k: cross(k).start())

        def piece(i, _):
            @pl.when(c == 0)
            def _():
                wo_copy(i).wait()

            t = _dot(seen_s[...], wo_s[i])
            send_s[late * n + i] = t[:half].astype(jnp.bfloat16)
            own_s[lax.rem(i, 2)] = t[half:]
            over(c, i).start()
            pl.when(i > 0)(lambda: finish(i - 1))

        lax.fori_loop(0, n, piece, None)
        finish(n - 1)
        for i in range(n):
            over(c, i).wait_send()
        for k in range(chunks):
            pl.when(c == k)(lambda k=k: [out(k, i).start() for i in range(n)] and None)

    lax.fori_loop(0, chunks, chunk, None)
    for c in range(chunks):
        for i in range(n):
            out(c, i).wait()
    for i in range(crossing):
        cross(i).wait_send()
        cross(i).wait_recv()


def _second(x_ref, *refs, parts, first, pieces):
    m = 1 + max(p[0] for p in parts)
    chips, others, (gain_ref, wg_ref, wu_ref, wd_ref, _), rest = refs[:m], refs[m : 2 * m], refs[2 * m : 2 * m + 5], refs[2 * m + 5 :]
    outs, mine_ref, (in_s, b_s, w_s, hidden_s, wd_s, send_s, recv_s, own_s, sum_s) = rest[:pieces], rest[pieces], rest[pieces + 1 : -9]
    in_sem, mine_sem, b_send_sem, b_recv_sem, w_sem, wd_sem, send_sem, recv_sem, out_sem = rest[-9:]
    rows, _ = b_s.shape
    half, wide, n = rows // 2, w_s.shape[2] // 2, send_s.shape[0]
    blocks = wg_ref.shape[1] // wide
    core, peer = _places()
    _greet(peer)

    def weight_copies(i):
        at = pl.ds(pl.multiple_of(i * wide, HEAD), wide)
        slot = lax.rem(i, 2)
        return [pltpu.make_async_copy(w.at[:, at], w_s.at[slot, :, pl.ds(m * wide, wide)], w_sem.at[m, slot]) for m, w in enumerate((wg_ref, wu_ref))]

    def down_copy(i):
        slot = lax.rem(i, 2)
        return pltpu.make_async_copy(wd_ref.at[:, pl.ds(pl.multiple_of(i * PIECE, PIECE), PIECE)], wd_s.at[slot], wd_sem.at[slot])

    load = half // 4
    count = half // len(parts)

    def inputs(i):
        part, at = divmod(i * load, count)
        array, row = parts[part]
        here = pl.ds(i * load, load)
        x = x_ref.at[pl.ds(pl.multiple_of(first + 2 * count * part + core * count + at, load), load), :]
        given = (x, chips[array].at[pl.ds(row + at, load), :], others[array].at[pl.ds(row + at, load), :])
        return [pltpu.make_async_copy(r, in_s.at[m, here, :], in_sem.at[m, i]) for m, r in enumerate(given)]

    def b_over(i):
        return _to_core(peer, b_s.at[pl.ds(half + i * load, load), :], b_s.at[pl.ds(i * load, load), :], b_send_sem.at[i], b_recv_sem.at[i])

    for i in range(4):
        for c in inputs(i):
            c.start()
    for i in range(2):
        for c in weight_copies(i):
            c.start()

    step = 16
    gain = gain_ref[...].astype(jnp.float32)
    pl.semaphore_wait(pltpu.get_barrier_semaphore(), 1)
    for i in range(4):
        for c in inputs(i):
            c.wait()

        def add(j, _):
            here = pl.ds(pl.multiple_of(i * load + j * step, step), step)
            x, a, b = (in_s[m, here, :].astype(jnp.float32) for m in range(3))
            h = (x + (a + b)).astype(jnp.bfloat16)
            in_s[0, here, :] = h
            b_s[pl.ds(pl.multiple_of(half + i * load + j * step, step), step), :] = _normed([h], [gain])[0]

        lax.fori_loop(0, load // step, add, None)
        b_over(i).start()
    kept = pltpu.make_async_copy(in_s.at[0], mine_ref, mine_sem)
    kept.start()
    for i in range(2):
        down_copy(i).start()
    for i in range(4):
        b_over(i).wait_recv()

    def block(i, _):
        slot = lax.rem(i, 2)
        for c in weight_copies(i):
            c.wait()
        both = _dot(b_s[...], w_s[slot])
        hidden_s[:, pl.ds(pl.multiple_of(i * wide, HEAD), wide)] = (jax.nn.silu(both[:, :wide]) * both[:, wide:]).astype(jnp.bfloat16)

        @pl.when(i + 2 < blocks)
        def _():
            for c in weight_copies(i + 2):
                c.start()

    lax.fori_loop(0, blocks, block, None)

    def term(i):
        down_copy(i).wait()
        t = _dot(hidden_s[...], wd_s[lax.rem(i, 2)])

        @pl.when(i + 2 < n)
        def _():
            down_copy(i + 2).start()

        return t

    _sum_on_chip(peer, term, outs, send_s, recv_s, own_s, sum_s, send_sem, recv_sem, out_sem)
    for i in range(4):
        b_over(i).wait_send()
    kept.wait()


def solution(mesh):
    def step(x, gain_a, wq, wk, wv, wo, gain_m, w_gate, w_up, w_down):
        batch, length, d = x.shape
        n, low, half = d // PIECE, jnp.bfloat16, CHUNK // 2
        chunks, per = batch * length // CHUNK, length // CHUNK
        core = lax.rem(lax.axis_index("tp"), 2)
        turns = rotary(length)
        x2 = x.reshape(batch * length, d)
        dma, anywhere, inside = pltpu.SemaphoreType.DMA, pl.BlockSpec(memory_space=pl.ANY), pl.BlockSpec(memory_space=pltpu.VMEM)
        array = lambda *shape: jax.ShapeDtypeStruct(shape, low)

        def over(t):
            return lax.ppermute(t, "tp", OTHER_CHIP)

        def first_half():
            width, both = 512, 2 * wk.shape[1]
            count = wq.shape[1] // width + 1
            crossing = GROUPS[0] * n
            return pl.pallas_call(
                functools.partial(_first, groups_of=GROUPS, crossing=crossing),
                in_specs=[anywhere, inside, inside, *[anywhere] * 4],
                out_specs=[anywhere] * (len(GROUPS) + 1),
                out_shape=[array(g * half, d) for g in GROUPS] + [array(GROUPS[0] * half, d)],
                scratch_shapes=[
                    pltpu.VMEM((2, CHUNK, d), low), pltpu.VMEM((CHUNK, d), low), pltpu.VMEM((count, d, width), low),
                    pltpu.VMEM((n, wo.shape[0], PIECE), low), pltpu.VMEM((count, CHUNK, width), low), pltpu.VMEM((length, both), low),
                    pltpu.VMEM((CHUNK, wo.shape[0]), low), pltpu.VMEM((2, length, HEAD), jnp.float32),
                    pltpu.VMEM((2 * n, half, PIECE), low), pltpu.VMEM((2 * n, half, PIECE), low), pltpu.VMEM((2, half, PIECE), jnp.float32),
                    pltpu.VMEM((chunks * n, half, PIECE), low),
                    dma((2,)), dma((count + 1,)), dma((n,)), dma((2 * n,)), dma((2 * n,)), dma((chunks * n,)), dma((crossing,)), dma((crossing,)),
                ],
                compiler_params=pltpu.CompilerParams(collective_id=0, has_side_effects=True, vmem_limit_bytes=VMEM),
                cost_estimate=pl.CostEstimate(flops=2 * batch * length * d * (2560 + 256), transcendentals=8 * batch * length * length, bytes_accessed=60 * 2**20),
                name="attention",
            )(x2, gain_a.reshape(1, d), turns, wq, wk, wv, wo)

        def second_half(s, chips, others, parts, after):
            wide, pieces, half = 640, 4 if s == batch - 1 else 1, length // 2
            return pl.pallas_call(
                functools.partial(_second, parts=parts, first=s * length, pieces=pieces),
                in_specs=[*[anywhere] * (1 + 2 * len(chips)), inside, *[anywhere] * 4],
                out_specs=[anywhere] * (pieces + 1),
                out_shape=[array(half, d // pieces)] * pieces + [array(half, d)],
                scratch_shapes=[
                    pltpu.VMEM((3, half, d), low), pltpu.VMEM((length, d), low), pltpu.VMEM((2, d, 2 * wide), low),
                    pltpu.VMEM((length, w_down.shape[0]), low), pltpu.VMEM((2, w_down.shape[0], PIECE), low),
                    pltpu.VMEM((n, half, PIECE), low), pltpu.VMEM((n, half, PIECE), low), pltpu.VMEM((2, half, PIECE), jnp.float32), pltpu.VMEM((n, half, PIECE), low),
                    dma((3, 4)), dma, dma((4,)), dma((4,)), dma((2, 2)), dma((2,)), dma((n,)), dma((n,)), dma((n,)),
                ],
                compiler_params=pltpu.CompilerParams(collective_id=1 + s, has_side_effects=True, vmem_limit_bytes=VMEM),
                cost_estimate=pl.CostEstimate(flops=6 * length * d * w_down.shape[0], transcendentals=length * w_down.shape[0], bytes_accessed=84 * 2**20),
            )(x2, *chips, *others, gain_m.reshape(1, d), w_gate, w_up, w_down, after)

        *sums, crossed = first_half()
        others = [crossed] + [over(t) for g, t in enumerate(sums) if g]
        after, ends = sums[-1], []
        for s in range(batch):
            where = [_group(GROUPS, c) for c in range(s * per, (s + 1) * per)]
            used = sorted({g for g, _ in where})
            parts = [(used.index(g), c * half) for g, c in where]
            *chips, mine = second_half(s, [sums[g] for g in used], [others[g] for g in used], parts, after)
            after = chips[0]
            ends.append((mine, chips, [over(chip) for chip in chips]))
        y = pl.pallas_call(lambda _, o: None, in_specs=[anywhere], out_specs=anywhere, out_shape=jax.ShapeDtypeStruct(x2.shape, low), name="empty")(after)
        y = y.reshape(batch, per, 2, half, d)
        for s, (mine, chips, others) in enumerate(ends):
            for j, (chip, other) in enumerate(zip(chips, others)):
                wide = d // len(chips)
                other, y = lax.optimization_barrier((other, y))
                t = (mine[:, j * wide : (j + 1) * wide].astype(jnp.float32) + (chip.astype(jnp.float32) + other.astype(jnp.float32))).astype(low)
                for rows, side in ((t, core), (lax.ppermute(t, "tp", SAME_CHIP), 1 - core)):
                    y = lax.dynamic_update_slice(y, rows.reshape(1, per, 1, half, wide), (s, 0, side, 0, j * wide))
        return y.reshape(x.shape)

    tokens, whole, columns, rows_of = P("dp", None, None), P(None), P(None, "tp"), P("tp", None)
    return jax.shard_map(
        step,
        mesh=mesh,
        in_specs=(tokens, whole, columns, columns, columns, rows_of, whole, columns, columns, rows_of),
        out_specs=tokens,
        check_vma=False,
    )
```

```python
import functools

import jax
import jax.numpy as jnp
import numpy as np
from jax import lax
from jax.experimental import pallas as pl
from jax.experimental.pallas import tpu as pltpu
from jax.sharding import PartitionSpec as P


HEAD = 128
THETA = 10000
LOG2E = 1.4426950408889634
SAME_CHIP = [(0, 1), (1, 0), (2, 3), (3, 2)]
OTHER_CHIP = [(0, 2), (2, 0), (1, 3), (3, 1)]
FINE = 16
ARRAYS = ((0, 3, 0, 4), (3, 1, 0, 4), (4, 2, 0, 4), (6, 2, 0, 4))
CROSSING = 1
CHUNK = 256
PIECE = 1024
VMEM = 63 * 2**20


def _dot(a, b, ca=1, cb=0):
    return lax.dot_general(a, b, (((ca,), (cb,)), ((), ())), preferred_element_type=jnp.float32)


def rotary(rows):
    half = HEAD // 2
    place = np.concatenate([np.arange(0, rows, FINE), np.arange(FINE)])
    angle = place[:, None] * float(THETA) ** (-np.arange(half) / half)
    return np.stack([np.tile(f(angle), 2) for f in (np.cos, np.sin)]).astype(np.float32)


def _turned(t, cos, sin):
    t = t.astype(jnp.float32)
    return (t * cos + pltpu.roll(t, HEAD // 2, 1) * sin).astype(jnp.bfloat16)


def _normed(parts, gains):
    wide = [p.astype(jnp.float32) for p in parts]
    total = sum(jnp.sum(w * w, -1, keepdims=True) for w in wide)
    scale = lax.rsqrt(total * (1 / sum(w.shape[1] for w in wide)) + 1e-6)
    return [(w * scale * g).astype(jnp.bfloat16) for w, g in zip(wide, gains)]


def _places():
    me = lax.axis_index("tp")
    core = lax.rem(me, 2)
    return core, me + 1 - 2 * core


def _greet(peer):
    pl.semaphore_signal(pltpu.get_barrier_semaphore(), inc=1, device_id={"tp": peer}, device_id_type=pl.DeviceIdType.MESH)


def _to_core(peer, src, dst, send, recv):
    return pltpu.make_async_remote_copy(
        src_ref=src, dst_ref=dst, send_sem=send, recv_sem=recv, device_id={"tp": peer}, device_id_type=pl.DeviceIdType.MESH
    )


def _sum_on_chip(peer, term, out_refs, send_s, recv_s, own_s, sum_s, send_sem, recv_sem, out_sem):
    n, rows = send_s.shape[0], send_s.shape[1]
    per = n // len(out_refs)

    def over(i):
        return _to_core(peer, send_s.at[i], recv_s.at[i], send_sem.at[i], recv_sem.at[i])

    def out(i):
        return pltpu.make_async_copy(sum_s.at[i], out_refs[i // per].at[:, pl.ds(i % per * PIECE, PIECE)], out_sem.at[i])

    def finish(i):
        over(i).wait_recv()
        sum_s[i] = (own_s[lax.rem(i, 2)] + recv_s[i].astype(jnp.float32)).astype(jnp.bfloat16)

    def piece(i, _):
        t = term(i)
        send_s[i] = t[:rows].astype(jnp.bfloat16)
        own_s[lax.rem(i, 2)] = t[rows:]
        over(i).start()

        @pl.when(i > 0)
        def _():
            finish(i - 1)

    lax.fori_loop(0, n, piece, None)
    for i in range(n - 1):
        out(i).start()
    finish(n - 1)
    out(n - 1).start()
    for i in range(n):
        over(i).wait_send()
        out(i).wait()


def _first(x_ref, gain_ref, turn_ref, wq_ref, wk_ref, wv_ref, wo_ref, *rest):
    chip_refs, other_refs, rest = rest[: len(ARRAYS)], rest[len(ARRAYS) : len(ARRAYS) + CROSSING], rest[len(ARRAYS) + CROSSING :]
    (x_s, a_s, w_s, wo_s, qkv_s, keys_s, seen_s, turn_s, send_s, recv_s, own_s, sum_s, gain_s, angle_s,
     small_sem, x_sem, w_sem, wo_sem, send_sem, recv_sem, out_sem, x_send_sem, x_recv_sem) = rest
    rows, d = a_s.shape
    half, width, n, chunks = rows // 2, w_s.shape[2], wo_s.shape[0], sum_s.shape[0] // wo_s.shape[0]
    groups = wk_ref.shape[1] // HEAD
    core, peer = _places()
    across = lax.rem(lax.axis_index("tp") + 2, 4)
    _greet(peer)
    _greet(across)

    weights = [pltpu.make_async_copy(w, w_s.at[0, :, pl.ds(i * width // 2, width // 2)], w_sem.at[i]) for i, w in enumerate((wk_ref, wv_ref))]
    weights += [pltpu.make_async_copy(wq_ref.at[:, pl.ds(i * width, width)], w_s.at[i + 1], w_sem.at[i + 2]) for i in range(w_s.shape[0] - 1)]

    def x_copy(c):
        return pltpu.make_async_copy(x_ref.at[pl.ds(pl.multiple_of(c * rows, rows), rows), :], x_s.at[lax.rem(c, 2)], x_sem.at[lax.rem(c, 2)])

    def wo_copy(i):
        return pltpu.make_async_copy(wo_ref.at[:, pl.ds(pl.multiple_of(i * PIECE, PIECE), PIECE)], wo_s.at[i], wo_sem.at[i])

    small = [pltpu.make_async_copy(r, t, small_sem.at[i]) for i, (r, t) in enumerate(((gain_ref, gain_s), (turn_ref, angle_s)))]
    for c in small:
        c.start()
    x_copy(0).start()
    for c in weights[:2]:
        c.start()

    step = 32
    e = HEAD**-0.5 * LOG2E
    hidden = lax.broadcasted_iota(jnp.int32, (rows, rows), 0) > lax.broadcasted_iota(jnp.int32, (rows, rows), 1)

    def over(c, i):
        slot = lax.rem(c, 2) * n + i
        return _to_core(peer, send_s.at[slot], recv_s.at[slot], send_sem.at[slot], recv_sem.at[slot])

    def place_in(array, ref, c, i):
        first, _, column, _ = ARRAYS[array]
        return ref.at[pl.ds(pl.multiple_of((c - first) * half, half), half), pl.ds(pl.multiple_of((i - column) * PIECE, PIECE), PIECE)]

    def cross(array, c, i):
        k = c * n + i
        return _to_core(across, sum_s.at[k], place_in(array, other_refs[array], c, i), x_send_sem.at[k], x_recv_sem.at[k])

    def out(array, c, i):
        return pltpu.make_async_copy(sum_s.at[c * n + i], place_in(array, chip_refs[array], c, i), out_sem.at[c * n + i])

    def finish(c, i):
        over(c, i).wait_recv()
        sum_s[c * n + i] = (own_s[i] + recv_s[lax.rem(c, 2) * n + i].astype(jnp.float32)).astype(jnp.bfloat16)
        for array, (first, count, column, pieces) in enumerate(ARRAYS[:CROSSING]):
            inside = (c >= first) & (c < first + count) & (i >= column) & (i < column + pieces)
            pl.when(inside)(lambda array=array: cross(array, c, i).start())

    def lag(c):
        return jnp.where(c == 0, 1, 2)

    def close(c):
        lax.fori_loop(n - lag(c), n, lambda i, _: finish(c, i), None)
        for i in range(n):
            over(c, i).wait_send()
        for array, (first, count, column, pieces) in enumerate(ARRAYS):

            @pl.when((c >= first) & (c < first + count))
            def _():
                for i in range(column, column + pieces):
                    out(array, c, i).start()

    def norm(slot, at):
        here = pl.ds(pl.multiple_of(at, step), step)
        a_s[here, :] = _normed([x_s[slot, here, :]], [gain])[0]

    small[0].wait()
    gain = gain_s[...].astype(jnp.float32).reshape(1, d)
    x_copy(0).wait()
    for c in weights[2:]:
        c.start()
    lax.fori_loop(0, rows // step, lambda j, _: norm(0, j * step), None)
    small[1].wait()
    sign = jnp.where(lax.broadcasted_iota(jnp.int32, (1, HEAD), 1) < HEAD // 2, -1.0, 1.0)
    coarse = angle_s.shape[1] - FINE
    cos, sin = angle_s[0, coarse:, :], angle_s[1, coarse:, :]
    for i in range(coarse):
        c, s = angle_s[0, i : i + 1, :], angle_s[1, i : i + 1, :]
        turn_s[0, i * FINE : (i + 1) * FINE, :] = cos * c - sin * s
        turn_s[1, i * FINE : (i + 1) * FINE, :] = (sin * c + cos * s) * sign
    for c in weights[:2]:
        c.wait()

    def chunk(c, _):
        late = lax.rem(c, 2)
        place = pl.multiple_of(late * rows, rows)

        @pl.when((c > 0) & (c + 1 < chunks))
        def _():
            x_copy(c + 1).start()

        def project(i, _):
            @pl.when((i > 0) & (c == 0))
            def _():
                pltpu.make_async_copy(wq_ref.at[:, pl.ds(0, width)], w_s.at[i], w_sem.at[i + 1]).wait()

            qkv_s[i] = _dot(a_s[...], w_s[i]).astype(jnp.bfloat16)

            @pl.when((i == 0) & (c == 0))
            def _():
                for k in range(n):
                    wo_copy(k).start()
                x_copy(1).start()

        lax.fori_loop(0, w_s.shape[0], project, None)

        @pl.when(c == 0)
        def _():
            pl.semaphore_wait(pltpu.get_barrier_semaphore(), 2)

        pl.when(c > 0)(lambda: close(c - 1))
        new = pl.ds(place, rows)
        for g in range(groups):
            keys_s[new, g * HEAD : (g + 1) * HEAD] = _turned(qkv_s[0, :, g * HEAD : (g + 1) * HEAD], turn_s[0, new, :], turn_s[1, new, :])
        keys_s[new, groups * HEAD :] = qkv_s[0, :, groups * HEAD :]

        def attend(g, _, before):
            total = before + rows
            k = keys_s[:total, pl.ds(pl.multiple_of(g * HEAD, HEAD), HEAD)]
            v = keys_s[:total, pl.ds(pl.multiple_of((g + groups) * HEAD, HEAD), HEAD)]
            values = jnp.concatenate([v.T, jnp.ones((8, total), jnp.bfloat16)], axis=0)
            scores = []
            for h in range(4):
                q = _turned(qkv_s[1 + g, :, h * HEAD : (h + 1) * HEAD], turn_s[0, before:total, :], turn_s[1, before:total, :])
                scores.append(_dot(k, q, 1, 1))
            found = []
            for s in scores:
                last = jnp.where(hidden, -1e30, s[before:])
                s = jnp.concatenate([s[:before], last], axis=0) if before else last
                found.append(jnp.exp2((s - s.max(axis=0, keepdims=True)) * e).astype(jnp.bfloat16))
            for h, p in enumerate(found):
                mix = _dot(values, p)
                got = (mix[:HEAD] * (1 / mix[HEAD : HEAD + 1])).T.astype(jnp.bfloat16)
                for part in range(2):
                    to = pl.ds(pl.multiple_of(jnp.where(core == part, half, 0), half), half)
                    seen_s[to, pl.ds(pl.multiple_of((g * 4 + h) * HEAD, HEAD), HEAD)] = got[part * half : (part + 1) * half]

        for p in range(2):
            pl.when(late == p)(lambda p=p: lax.fori_loop(0, groups, functools.partial(attend, before=p * rows), None))

        pl.when(c + 1 < chunks)(lambda: x_copy(c + 1).wait())

        def piece(i, _):
            @pl.when(c == 0)
            def _():
                wo_copy(i).wait()

            for j in range(rows // n // step):
                norm(1 - late, (i * (rows // n // step) + j) * step)
            t = _dot(seen_s[...], wo_s[i])
            send_s[late * n + i] = t[:half].astype(jnp.bfloat16)
            own_s[i] = t[half:]
            over(c, i).start()
            pl.when(i >= lag(c))(lambda: finish(c, i - lag(c)))

        lax.fori_loop(0, n, piece, None)

    lax.fori_loop(0, chunks, chunk, None)
    close(chunks - 1)
    for array, (first, count, column, pieces) in enumerate(ARRAYS):

        def done(k, _):
            c, i = first + lax.div(k, pieces), column + lax.rem(k, pieces)
            out(array, c, i).wait()
            if array < CROSSING:
                cross(array, c, i).wait_send()
                cross(array, c, i).wait_recv()

        lax.fori_loop(0, count * pieces, done, None)


def _second(x_ref, *refs, parts, first, pieces):
    m = 1 + max(p[0] for part in parts for p in part)
    chips, others, (gain_ref, wg_ref, wu_ref, wd_ref, _), rest = refs[:m], refs[m : 2 * m], refs[2 * m : 2 * m + 5], refs[2 * m + 5 :]
    outs, mine_ref, (in_s, b_s, w_s, both_s, hidden_s, wd_s, send_s, recv_s, own_s, sum_s) = rest[:pieces], rest[pieces], rest[pieces + 1 : -9]
    in_sem, mine_sem, b_send_sem, b_recv_sem, w_sem, wd_sem, send_sem, recv_sem, out_sem = rest[-9:]
    rows, d = b_s.shape
    half, wide, n = rows // 2, w_s.shape[2] // 2, send_s.shape[0]
    blocks = wg_ref.shape[1] // wide
    core, peer = _places()
    _greet(peer)

    def weight_copies(i):
        at = pl.ds(pl.multiple_of(i * wide, HEAD), wide)
        slot = lax.rem(i, 2)
        return [pltpu.make_async_copy(w.at[:, at], w_s.at[slot, :, pl.ds(m * wide, wide)], w_sem.at[m, slot]) for m, w in enumerate((wg_ref, wu_ref))]

    def down_copy(i):
        slot = lax.rem(i, 2)
        return pltpu.make_async_copy(wd_ref.at[:, pl.ds(pl.multiple_of(i * PIECE, PIECE), PIECE)], wd_s.at[slot], wd_sem.at[slot])

    load = half // 4
    count = half // len(parts)

    def inputs(i):
        here = pl.ds(pl.multiple_of(i * load, load), load)
        return [pltpu.make_async_copy(x_ref.at[pl.ds(0, load), :], in_s.at[m, here, :], in_sem.at[m, i]) for m in range(3)]

    def fetch(i):
        part, at = divmod(i * load, count)
        here = pl.ds(i * load, load)
        x = x_ref.at[pl.ds(pl.multiple_of(first + 2 * count * part + core * count + at, load), load), :]
        pltpu.make_async_copy(x, in_s.at[0, here, :], in_sem.at[0, i]).start()
        for array, row, column, pieces in parts[part]:
            for m, given in ((1, chips), (2, others)):
                to = in_s.at[m, here, pl.ds(column * PIECE, pieces * PIECE)]
                pltpu.make_async_copy(given[array].at[pl.ds(row + at, load), :], to, in_sem.at[m, i]).start()

    def b_over(i):
        at = pl.multiple_of(i * load, load)
        return _to_core(peer, b_s.at[pl.ds(half + at, load), :], b_s.at[pl.ds(at, load), :], b_send_sem.at[i], b_recv_sem.at[i])

    for i in range(4):
        fetch(i)
    for i in range(2):
        for c in weight_copies(i):
            c.start()

    step = 16
    gain = gain_ref[...].astype(jnp.float32).reshape(1, d)
    pl.semaphore_wait(pltpu.get_barrier_semaphore(), 1)

    def adds(i, _):
        for c in inputs(i):
            c.wait()

        def add(j, _):
            here = pl.ds(pl.multiple_of(i * load + j * step, step), step)
            x, a, b = (in_s[m, here, :].astype(jnp.float32) for m in range(3))
            h = (x + (a + b)).astype(jnp.bfloat16)
            in_s[0, here, :] = h
            b_s[pl.ds(pl.multiple_of(half + i * load + j * step, step), step), :] = _normed([h], [gain])[0]

        lax.fori_loop(0, load // step, add, None)
        b_over(i).start()

    lax.fori_loop(0, 4, adds, None)
    kept = pltpu.make_async_copy(in_s.at[0], mine_ref, mine_sem)
    kept.start()
    for i in range(2):
        down_copy(i).start()
    for i in range(4):
        b_over(i).wait_recv()

    def gated(i):
        hidden_s[:, pl.ds(pl.multiple_of(i * wide, HEAD), wide)] = (jax.nn.silu(both_s[:, :wide]) * both_s[:, wide:]).astype(jnp.bfloat16)

    def block(i, _):
        slot = lax.rem(i, 2)
        for c in weight_copies(i):
            c.wait()
        gated(jnp.maximum(i - 1, 0))
        both_s[...] = _dot(b_s[...], w_s[slot])

        @pl.when(i + 2 < blocks)
        def _():
            for c in weight_copies(i + 2):
                c.start()

    lax.fori_loop(0, blocks, block, None)
    gated(blocks - 1)

    def term(i):
        down_copy(i).wait()
        t = _dot(hidden_s[...], wd_s[lax.rem(i, 2)])

        @pl.when(i + 2 < n)
        def _():
            down_copy(i + 2).start()

        return t

    _sum_on_chip(peer, term, outs, send_s, recv_s, own_s, sum_s, send_sem, recv_sem, out_sem)
    for i in range(4):
        b_over(i).wait_send()
    kept.wait()


def solution(mesh):
    def step(x, gain_a, wq, wk, wv, wo, gain_m, w_gate, w_up, w_down):
        batch, length, d = x.shape
        n, low, half = d // PIECE, jnp.bfloat16, CHUNK // 2
        chunks, per = batch * length // CHUNK, length // CHUNK
        core = lax.rem(lax.axis_index("tp"), 2)
        turns = rotary(length)
        x2 = x.reshape(batch * length, d)
        dma, anywhere, inside = pltpu.SemaphoreType.DMA, pl.BlockSpec(memory_space=pl.ANY), pl.BlockSpec(memory_space=pltpu.VMEM)
        array = lambda *shape: jax.ShapeDtypeStruct(shape, low)

        def over(t):
            return lax.ppermute(t, "tp", OTHER_CHIP)

        def first_half():
            width, both = 512, 2 * wk.shape[1]
            count = wq.shape[1] // width + 1
            sums = [array(chunks * half, pieces * PIECE) for _, chunks, _, pieces in ARRAYS]
            return pl.pallas_call(
                _first,
                in_specs=[anywhere] * 7,
                out_specs=[anywhere] * (len(ARRAYS) + CROSSING),
                out_shape=[*sums, *sums[:CROSSING]],
                scratch_shapes=[
                    pltpu.VMEM((2, CHUNK, d), low), pltpu.VMEM((CHUNK, d), low), pltpu.VMEM((count, d, width), low),
                    pltpu.VMEM((n, wo.shape[0], PIECE), low), pltpu.VMEM((count, CHUNK, width), low), pltpu.VMEM((length, both), low),
                    pltpu.VMEM((CHUNK, wo.shape[0]), low), pltpu.VMEM((2, length, HEAD), jnp.float32),
                    pltpu.VMEM((2 * n, half, PIECE), low), pltpu.VMEM((2 * n, half, PIECE), low), pltpu.VMEM((n, half, PIECE), jnp.float32),
                    pltpu.VMEM((chunks * n, half, PIECE), low), pltpu.VMEM((d,), low), pltpu.VMEM(turns.shape, jnp.float32),
                    dma((2,)), dma((2,)), dma((count + 1,)), dma((n,)), dma((2 * n,)), dma((2 * n,)), dma((chunks * n,)), dma((chunks * n,)), dma((chunks * n,)),
                ],
                compiler_params=pltpu.CompilerParams(collective_id=0, has_side_effects=True, vmem_limit_bytes=VMEM),
                cost_estimate=pl.CostEstimate(flops=2 * batch * length * d * (2560 + 256), transcendentals=8 * batch * length * length, bytes_accessed=60 * 2**20),
                name="attention",
            )(x2, gain_a, turns, wq, wk, wv, wo)

        def second_half(s, chips, others, parts, after):
            wide, pieces, half = 640, 4 if s == batch - 1 else 1, length // 2
            return pl.pallas_call(
                functools.partial(_second, parts=parts, first=s * length, pieces=pieces),
                in_specs=[*[anywhere] * (1 + 2 * len(chips)), inside, *[anywhere] * 4],
                out_specs=[anywhere] * (pieces + 1),
                out_shape=[array(half, d // pieces)] * pieces + [array(half, d)],
                scratch_shapes=[
                    pltpu.VMEM((3, half, d), low), pltpu.VMEM((length, d), low), pltpu.VMEM((2, d, 2 * wide), low), pltpu.VMEM((length, 2 * wide), jnp.float32),
                    pltpu.VMEM((length, w_down.shape[0]), low), pltpu.VMEM((2, w_down.shape[0], PIECE), low),
                    pltpu.VMEM((n, half, PIECE), low), pltpu.VMEM((n, half, PIECE), low), pltpu.VMEM((2, half, PIECE), jnp.float32), pltpu.VMEM((n, half, PIECE), low),
                    dma((3, 4)), dma, dma((4,)), dma((4,)), dma((2, 2)), dma((2,)), dma((n,)), dma((n,)), dma((n,)),
                ],
                compiler_params=pltpu.CompilerParams(collective_id=1 + s, has_side_effects=True, vmem_limit_bytes=VMEM),
                cost_estimate=pl.CostEstimate(flops=6 * length * d * w_down.shape[0], transcendentals=length * w_down.shape[0], bytes_accessed=84 * 2**20),
            )(x2, *chips, *others, gain_m, w_gate, w_up, w_down, after)

        got = first_half()
        sums, others = got[: len(ARRAYS)], [*got[len(ARRAYS) :]]
        others += [over(t) for k, t in enumerate(sums) if k >= CROSSING]
        after, ends = sums[-1], []
        for s in range(batch):
            found = [[(k, c - a[0], a) for k, a in enumerate(ARRAYS) if a[0] <= c < a[0] + a[1]] for c in range(s * per, (s + 1) * per)]
            used = sorted({f[0] for part in found for f in part})
            parts = [[(used.index(k), c * half, a[2], a[3]) for k, c, a in part] for part in found]
            *chips, mine = second_half(s, [sums[k] for k in used], [others[k] for k in used], parts, after)
            after = chips[0]
            ends.append((mine, chips, [over(chip) for chip in chips]))
        y = pl.pallas_call(lambda _, o: None, in_specs=[anywhere], out_specs=anywhere, out_shape=jax.ShapeDtypeStruct(x2.shape, low), name="empty")(after)
        y = y.reshape(batch, per, 2, half, d)
        for s, (mine, chips, others) in enumerate(ends):
            for j, (chip, other) in enumerate(zip(chips, others)):
                wide = d // len(chips)
                other, y = lax.optimization_barrier((other, y))
                t = (mine[:, j * wide : (j + 1) * wide].astype(jnp.float32) + (chip.astype(jnp.float32) + other.astype(jnp.float32))).astype(low)
                for rows, side in ((t, core), (lax.ppermute(t, "tp", SAME_CHIP), 1 - core)):
                    y = lax.dynamic_update_slice(y, rows.reshape(1, per, 1, half, wide), (s, 0, side, 0, j * wide))
        return y.reshape(x.shape)

    tokens, whole, columns, rows_of = P("dp", None, None), P(None), P(None, "tp"), P("tp", None)
    return jax.shard_map(
        step,
        mesh=mesh,
        in_specs=(tokens, whole, columns, columns, columns, rows_of, whole, columns, columns, rows_of),
        out_specs=tokens,
        check_vma=False,
    )
```

```python
import functools

import jax
import jax.numpy as jnp
import numpy as np
from jax import lax
from jax.experimental import pallas as pl
from jax.experimental.pallas import tpu as pltpu
from jax.sharding import PartitionSpec as P


HEAD = 128
THETA = 10000
LOG2E = 1.4426950408889634
SAME_CHIP = [(0, 1), (1, 0), (2, 3), (3, 2)]
OTHER_CHIP = [(0, 2), (2, 0), (1, 3), (3, 1)]
FINE = 16
ARRAYS = ((0, 3, 0, 4), (3, 1, 0, 4), (4, 2, 0, 4), (6, 2, 0, 4))
CROSSING = 1
LAST = (1024, 1024, 1024, 512, 512)
CHUNK = 256
PIECE = 1024
VMEM = 63 * 2**20


def _dot(a, b, ca=1, cb=0):
    return lax.dot_general(a, b, (((ca,), (cb,)), ((), ())), preferred_element_type=jnp.float32)


def rotary(rows):
    half = HEAD // 2
    place = np.concatenate([np.arange(0, rows, FINE), np.arange(FINE)])
    angle = place[:, None] * float(THETA) ** (-np.arange(half) / half)
    return np.stack([np.tile(f(angle), 2) for f in (np.cos, np.sin)]).astype(np.float32)


def _turned(t, cos, sin):
    t = t.astype(jnp.float32)
    return (t * cos + pltpu.roll(t, HEAD // 2, 1) * sin).astype(jnp.bfloat16)


def _normed(parts, gains):
    wide = [p.astype(jnp.float32) for p in parts]
    total = sum(jnp.sum(w * w, -1, keepdims=True) for w in wide)
    scale = lax.rsqrt(total * (1 / sum(w.shape[1] for w in wide)) + 1e-6)
    return [(w * scale * g).astype(jnp.bfloat16) for w, g in zip(wide, gains)]


def _places():
    me = lax.axis_index("tp")
    core = lax.rem(me, 2)
    return core, me + 1 - 2 * core


def _greet(peer):
    pl.semaphore_signal(pltpu.get_barrier_semaphore(), inc=1, device_id={"tp": peer}, device_id_type=pl.DeviceIdType.MESH)


def _to_core(peer, src, dst, send, recv):
    return pltpu.make_async_remote_copy(
        src_ref=src, dst_ref=dst, send_sem=send, recv_sem=recv, device_id={"tp": peer}, device_id_type=pl.DeviceIdType.MESH
    )


def _sum_on_chip(peer, term, out_refs, send_s, recv_s, own_s, sum_s, send_sem, recv_sem, out_sem):
    n, rows = send_s.shape[0], send_s.shape[1]

    def over(i):
        return _to_core(peer, send_s.at[i], recv_s.at[i], send_sem.at[i], recv_sem.at[i])

    def out(i):
        copies, first = [], 0
        for k, ref in enumerate(out_refs):
            last = first + ref.shape[1]
            low, high = max(first, i * PIECE), min(last, (i + 1) * PIECE)
            if low < high:
                here = sum_s.at[i, :, pl.ds(low - i * PIECE, high - low)]
                copies.append(pltpu.make_async_copy(here, ref.at[:, pl.ds(low - first, high - low)], out_sem.at[i, k]))
            first = last
        return copies

    def finish(i):
        over(i).wait_recv()
        sum_s[i] = (own_s[lax.rem(i, 2)] + recv_s[i].astype(jnp.float32)).astype(jnp.bfloat16)

    def piece(i, _):
        t = term(i)
        send_s[i] = t[:rows].astype(jnp.bfloat16)
        own_s[lax.rem(i, 2)] = t[rows:]
        over(i).start()

        @pl.when(i > 0)
        def _():
            finish(i - 1)

    lax.fori_loop(0, n, piece, None)
    for i in range(n):
        if i == n - 1:
            finish(i)
        for c in out(i):
            c.start()
    for i in range(n):
        over(i).wait_send()
        for c in out(i):
            c.wait()


def _first(x_ref, gain_ref, turn_ref, wq_ref, wk_ref, wv_ref, wo_ref, *rest):
    chip_refs, other_refs, rest = rest[: len(ARRAYS)], rest[len(ARRAYS) : len(ARRAYS) + CROSSING], rest[len(ARRAYS) + CROSSING :]
    (x_s, a_s, w_s, wo_s, qkv_s, keys_s, seen_s, turn_s, send_s, recv_s, own_s, sum_s, gain_s, angle_s,
     small_sem, x_sem, w_sem, wo_sem, send_sem, recv_sem, out_sem, x_send_sem, x_recv_sem) = rest
    rows, d = a_s.shape
    half, width, n, chunks = rows // 2, w_s.shape[2], wo_s.shape[0], sum_s.shape[0] // wo_s.shape[0]
    groups = wk_ref.shape[1] // HEAD
    core, peer = _places()
    across = lax.rem(lax.axis_index("tp") + 2, 4)
    _greet(peer)
    _greet(across)

    def fetch(w, to, sem):
        for r in range(0, d, d // 4):
            pltpu.make_async_copy(w.at[pl.ds(r, d // 4), :], to.at[pl.ds(r, d // 4), :], sem).start()


    def x_copy(c):
        return pltpu.make_async_copy(x_ref.at[pl.ds(pl.multiple_of(c * rows, rows), rows), :], x_s.at[lax.rem(c, 2)], x_sem.at[lax.rem(c, 2)])

    def x_part(i):
        here = pl.ds(pl.multiple_of(i * (rows // 4), rows // 4), rows // 4)
        return pltpu.make_async_copy(x_ref.at[here, :], x_s.at[0, here, :], x_sem.at[2 + i])

    def wo_copy(i):
        return pltpu.make_async_copy(wo_ref.at[:, pl.ds(pl.multiple_of(i * PIECE, PIECE), PIECE)], wo_s.at[i], wo_sem.at[i])

    small = [pltpu.make_async_copy(r, t, small_sem.at[i]) for i, (r, t) in enumerate(((gain_ref, gain_s), (turn_ref, angle_s)))]
    for c in small:
        c.start()
    for i in range(4):
        x_part(i).start()
    for i, w in enumerate((wk_ref, wv_ref)):
        fetch(w, w_s.at[0, :, pl.ds(i * width // 2, width // 2)], w_sem.at[0])

    step = 32
    e = HEAD**-0.5 * LOG2E
    hidden = lax.broadcasted_iota(jnp.int32, (rows, rows), 0) > lax.broadcasted_iota(jnp.int32, (rows, rows), 1)

    def over(c, i):
        slot = lax.rem(c, 2) * n + i
        return _to_core(peer, send_s.at[slot], recv_s.at[slot], send_sem.at[slot], recv_sem.at[slot])

    def place_in(array, ref, c, i):
        first, _, column, _ = ARRAYS[array]
        return ref.at[pl.ds(pl.multiple_of((c - first) * half, half), half), pl.ds(pl.multiple_of((i - column) * PIECE, PIECE), PIECE)]

    def cross(array, c, i):
        k = c * n + i
        return _to_core(across, sum_s.at[k], place_in(array, other_refs[array], c, i), x_send_sem.at[k], x_recv_sem.at[k])

    def out(array, c, i):
        return pltpu.make_async_copy(sum_s.at[c * n + i], place_in(array, chip_refs[array], c, i), out_sem.at[c * n + i])

    def finish(c, i):
        over(c, i).wait_recv()
        sum_s[c * n + i] = (own_s[i] + recv_s[lax.rem(c, 2) * n + i].astype(jnp.float32)).astype(jnp.bfloat16)
        for array, (first, count, column, pieces) in enumerate(ARRAYS[:CROSSING]):
            inside = (c >= first) & (c < first + count) & (i >= column) & (i < column + pieces)
            pl.when(inside)(lambda array=array: cross(array, c, i).start())

    def lag(c):
        return jnp.where(c == 0, 1, 2)

    def close(c):
        lax.fori_loop(n - lag(c), n, lambda i, _: finish(c, i), None)
        for i in range(n):
            over(c, i).wait_send()
        for array, (first, count, column, pieces) in enumerate(ARRAYS):

            @pl.when((c >= first) & (c < first + count))
            def _():
                for i in range(column, column + pieces):
                    out(array, c, i).start()

    def norm(slot, at):
        here = pl.ds(pl.multiple_of(at, step), step)
        a_s[here, :] = _normed([x_s[slot, here, :]], [gain])[0]

    small[0].wait()
    gain = gain_s[...].astype(jnp.float32).reshape(1, d)
    for i in range(w_s.shape[0] - 1):
        fetch(wq_ref.at[:, pl.ds(i * width, width)], w_s.at[i + 1], w_sem.at[i + 1])

    def early(i, _):
        x_part(i).wait()
        lax.fori_loop(0, rows // 4 // step, lambda j, _: norm(0, i * (rows // 4) + j * step), None)

    lax.fori_loop(0, 4, early, None)
    small[1].wait()
    sign = jnp.where(lax.broadcasted_iota(jnp.int32, (1, HEAD), 1) < HEAD // 2, -1.0, 1.0)
    coarse = angle_s.shape[1] - FINE
    cos, sin = angle_s[0, coarse:, :], angle_s[1, coarse:, :]
    for i in range(coarse):
        c, s = angle_s[0, i : i + 1, :], angle_s[1, i : i + 1, :]
        turn_s[0, i * FINE : (i + 1) * FINE, :] = cos * c - sin * s
        turn_s[1, i * FINE : (i + 1) * FINE, :] = (sin * c + cos * s) * sign

    def chunk(c, _):
        late = lax.rem(c, 2)
        place = pl.multiple_of(late * rows, rows)

        @pl.when((c > 0) & (c + 1 < chunks))
        def _():
            x_copy(c + 1).start()

        def project(i, _):
            @pl.when(c == 0)
            def _():
                pltpu.make_async_copy(wq_ref.at[:, pl.ds(0, width)], w_s.at[i], w_sem.at[i]).wait()

            qkv_s[i] = _dot(a_s[...], w_s[i]).astype(jnp.bfloat16)

            @pl.when((i < 2) & (c == 0))
            def _():
                wo_copy(2 * i).start()
                wo_copy(2 * i + 1).start()
                pl.when(i == 1)(lambda: x_copy(1).start())

        lax.fori_loop(0, w_s.shape[0], project, None)

        @pl.when(c == 0)
        def _():
            pl.semaphore_wait(pltpu.get_barrier_semaphore(), 2)

        pl.when(c > 0)(lambda: close(c - 1))
        new = pl.ds(place, rows)
        for g in range(groups):
            keys_s[new, g * HEAD : (g + 1) * HEAD] = _turned(qkv_s[0, :, g * HEAD : (g + 1) * HEAD], turn_s[0, new, :], turn_s[1, new, :])
        keys_s[new, groups * HEAD :] = qkv_s[0, :, groups * HEAD :]

        def attend(g, _, before):
            total = before + rows
            k = keys_s[:total, pl.ds(pl.multiple_of(g * HEAD, HEAD), HEAD)]
            v = keys_s[:total, pl.ds(pl.multiple_of((g + groups) * HEAD, HEAD), HEAD)]
            values = jnp.concatenate([v.T, jnp.ones((8, total), jnp.bfloat16)], axis=0)
            scores = []
            for h in range(4):
                q = _turned(qkv_s[1 + g, :, h * HEAD : (h + 1) * HEAD], turn_s[0, before:total, :], turn_s[1, before:total, :])
                scores.append(_dot(k, q, 1, 1))
            found = []
            for s in scores:
                last = jnp.where(hidden, -1e30, s[before:])
                s = jnp.concatenate([s[:before], last], axis=0) if before else last
                found.append(jnp.exp2((s - s.max(axis=0, keepdims=True)) * e).astype(jnp.bfloat16))
            for h, p in enumerate(found):
                mix = _dot(values, p)
                got = (mix[:HEAD] * (1 / mix[HEAD : HEAD + 1])).T.astype(jnp.bfloat16)
                for part in range(2):
                    to = pl.ds(pl.multiple_of(jnp.where(core == part, half, 0), half), half)
                    seen_s[to, pl.ds(pl.multiple_of((g * 4 + h) * HEAD, HEAD), HEAD)] = got[part * half : (part + 1) * half]

        for p in range(2):
            pl.when(late == p)(lambda p=p: lax.fori_loop(0, groups, functools.partial(attend, before=p * rows), None))

        pl.when(c + 1 < chunks)(lambda: x_copy(c + 1).wait())

        def piece(i, _):
            @pl.when(c == 0)
            def _():
                wo_copy(i).wait()

            for j in range(rows // n // step):
                norm(1 - late, (i * (rows // n // step) + j) * step)
            t = _dot(seen_s[...], wo_s[i])
            send_s[late * n + i] = t[:half].astype(jnp.bfloat16)
            own_s[i] = t[half:]
            over(c, i).start()
            pl.when(i >= lag(c))(lambda: finish(c, i - lag(c)))

        lax.fori_loop(0, n, piece, None)

    lax.fori_loop(0, chunks, chunk, None)
    close(chunks - 1)
    for array, (first, count, column, pieces) in enumerate(ARRAYS):

        def done(k, _):
            c, i = first + lax.div(k, pieces), column + lax.rem(k, pieces)
            out(array, c, i).wait()
            if array < CROSSING:
                cross(array, c, i).wait_send()
                cross(array, c, i).wait_recv()

        lax.fori_loop(0, count * pieces, done, None)


def _second(x_ref, *refs, parts, first, pieces):
    m = 1 + max(p[0] for part in parts for p in part)
    chips, others, (gain_ref, wg_ref, wu_ref, wd_ref, _), rest = refs[:m], refs[m : 2 * m], refs[2 * m : 2 * m + 5], refs[2 * m + 5 :]
    outs, mine_ref, (in_s, b_s, w_s, both_s, hidden_s, wd_s, send_s, recv_s, own_s, sum_s) = rest[:pieces], rest[pieces], rest[pieces + 1 : -9]
    in_sem, mine_sem, b_send_sem, b_recv_sem, w_sem, wd_sem, send_sem, recv_sem, out_sem = rest[-9:]
    rows, d = b_s.shape
    half, wide, n = rows // 2, w_s.shape[2] // 2, send_s.shape[0]
    blocks = wg_ref.shape[1] // wide
    core, peer = _places()
    _greet(peer)

    def weight_copies(i):
        at = pl.ds(pl.multiple_of(i * wide, HEAD), wide)
        slot = lax.rem(i, 2)
        return [pltpu.make_async_copy(w.at[:, at], w_s.at[slot, :, pl.ds(m * wide, wide)], w_sem.at[m, slot]) for m, w in enumerate((wg_ref, wu_ref))]

    def down_copy(i):
        slot = lax.rem(i, 2)
        return pltpu.make_async_copy(wd_ref.at[:, pl.ds(pl.multiple_of(i * PIECE, PIECE), PIECE)], wd_s.at[slot], wd_sem.at[slot])

    load = half // 4
    count = half // len(parts)

    def inputs(i):
        here = pl.ds(pl.multiple_of(i * load, load), load)
        return [pltpu.make_async_copy(x_ref.at[pl.ds(0, load), :], in_s.at[m, here, :], in_sem.at[m, i]) for m in range(3)]

    def fetch(i):
        part, at = divmod(i * load, count)
        here = pl.ds(i * load, load)
        x = x_ref.at[pl.ds(pl.multiple_of(first + 2 * count * part + core * count + at, load), load), :]
        pltpu.make_async_copy(x, in_s.at[0, here, :], in_sem.at[0, i]).start()
        for array, row, column, pieces in parts[part]:
            for m, given in ((1, chips), (2, others)):
                to = in_s.at[m, here, pl.ds(column * PIECE, pieces * PIECE)]
                pltpu.make_async_copy(given[array].at[pl.ds(row + at, load), :], to, in_sem.at[m, i]).start()

    def b_over(i):
        at = pl.multiple_of(i * load, load)
        return _to_core(peer, b_s.at[pl.ds(half + at, load), :], b_s.at[pl.ds(at, load), :], b_send_sem.at[i], b_recv_sem.at[i])

    for i in range(4):
        fetch(i)
    for i in range(2):
        for c in weight_copies(i):
            c.start()

    step = 16
    gain = gain_ref[...].astype(jnp.float32).reshape(1, d)
    pl.semaphore_wait(pltpu.get_barrier_semaphore(), 1)

    def adds(i, _):
        for c in inputs(i):
            c.wait()

        def add(j, _):
            here = pl.ds(pl.multiple_of(i * load + j * step, step), step)
            x, a, b = (in_s[m, here, :].astype(jnp.float32) for m in range(3))
            h = (x + (a + b)).astype(jnp.bfloat16)
            in_s[0, here, :] = h
            b_s[pl.ds(pl.multiple_of(half + i * load + j * step, step), step), :] = _normed([h], [gain])[0]

        lax.fori_loop(0, load // step, add, None)
        b_over(i).start()

    lax.fori_loop(0, 4, adds, None)
    kept = pltpu.make_async_copy(in_s.at[0], mine_ref, mine_sem)
    kept.start()
    for i in range(2):
        down_copy(i).start()
    for i in range(4):
        b_over(i).wait_recv()

    def gated(i):
        hidden_s[:, pl.ds(pl.multiple_of(i * wide, HEAD), wide)] = (jax.nn.silu(both_s[:, :wide]) * both_s[:, wide:]).astype(jnp.bfloat16)

    def block(i, _):
        slot = lax.rem(i, 2)
        for c in weight_copies(i):
            c.wait()
        gated(jnp.maximum(i - 1, 0))
        both_s[...] = _dot(b_s[...], w_s[slot])

        @pl.when(i + 2 < blocks)
        def _():
            for c in weight_copies(i + 2):
                c.start()

    lax.fori_loop(0, blocks, block, None)
    gated(blocks - 1)

    def term(i):
        down_copy(i).wait()
        t = _dot(hidden_s[...], wd_s[lax.rem(i, 2)])

        @pl.when(i + 2 < n)
        def _():
            down_copy(i + 2).start()

        return t

    _sum_on_chip(peer, term, outs, send_s, recv_s, own_s, sum_s, send_sem, recv_sem, out_sem)
    for i in range(4):
        b_over(i).wait_send()
    kept.wait()


def solution(mesh):
    def step(x, gain_a, wq, wk, wv, wo, gain_m, w_gate, w_up, w_down):
        batch, length, d = x.shape
        n, low, half = d // PIECE, jnp.bfloat16, CHUNK // 2
        chunks, per = batch * length // CHUNK, length // CHUNK
        core = lax.rem(lax.axis_index("tp"), 2)
        turns = rotary(length)
        x2 = x.reshape(batch * length, d)
        dma, anywhere, inside = pltpu.SemaphoreType.DMA, pl.BlockSpec(memory_space=pl.ANY), pl.BlockSpec(memory_space=pltpu.VMEM)
        array = lambda *shape: jax.ShapeDtypeStruct(shape, low)

        def over(t):
            return lax.ppermute(t, "tp", OTHER_CHIP)

        def first_half():
            width, both = 512, 2 * wk.shape[1]
            count = wq.shape[1] // width + 1
            sums = [array(chunks * half, pieces * PIECE) for _, chunks, _, pieces in ARRAYS]
            return pl.pallas_call(
                _first,
                in_specs=[anywhere] * 7,
                out_specs=[anywhere] * (len(ARRAYS) + CROSSING),
                out_shape=[*sums, *sums[:CROSSING]],
                scratch_shapes=[
                    pltpu.VMEM((2, CHUNK, d), low), pltpu.VMEM((CHUNK, d), low), pltpu.VMEM((count, d, width), low),
                    pltpu.VMEM((n, wo.shape[0], PIECE), low), pltpu.VMEM((count, CHUNK, width), low), pltpu.VMEM((length, both), low),
                    pltpu.VMEM((CHUNK, wo.shape[0]), low), pltpu.VMEM((2, length, HEAD), jnp.float32),
                    pltpu.VMEM((2 * n, half, PIECE), low), pltpu.VMEM((2 * n, half, PIECE), low), pltpu.VMEM((n, half, PIECE), jnp.float32),
                    pltpu.VMEM((chunks * n, half, PIECE), low), pltpu.VMEM((d,), low), pltpu.VMEM(turns.shape, jnp.float32),
                    dma((2,)), dma((6,)), dma((count,)), dma((n,)), dma((2 * n,)), dma((2 * n,)), dma((chunks * n,)), dma((chunks * n,)), dma((chunks * n,)),
                ],
                compiler_params=pltpu.CompilerParams(collective_id=0, has_side_effects=True, vmem_limit_bytes=VMEM),
                cost_estimate=pl.CostEstimate(flops=2 * batch * length * d * (2560 + 256), transcendentals=8 * batch * length * length, bytes_accessed=60 * 2**20),
                name="attention",
            )(x2, gain_a, turns, wq, wk, wv, wo)

        def second_half(s, chips, others, parts, after):
            wide, widths, half = 640, LAST if s == batch - 1 else (d,), length // 2
            pieces = len(widths)
            return pl.pallas_call(
                functools.partial(_second, parts=parts, first=s * length, pieces=pieces),
                in_specs=[*[anywhere] * (1 + 2 * len(chips)), inside, *[anywhere] * 4],
                out_specs=[anywhere] * (pieces + 1),
                out_shape=[*(array(half, w) for w in widths), array(half, d)],
                scratch_shapes=[
                    pltpu.VMEM((3, half, d), low), pltpu.VMEM((length, d), low), pltpu.VMEM((2, d, 2 * wide), low), pltpu.VMEM((length, 2 * wide), jnp.float32),
                    pltpu.VMEM((length, w_down.shape[0]), low), pltpu.VMEM((2, w_down.shape[0], PIECE), low),
                    pltpu.VMEM((n, half, PIECE), low), pltpu.VMEM((n, half, PIECE), low), pltpu.VMEM((2, half, PIECE), jnp.float32), pltpu.VMEM((n, half, PIECE), low),
                    dma((3, 4)), dma, dma((4,)), dma((4,)), dma((2, 2)), dma((2,)), dma((n,)), dma((n,)), dma((n, pieces)),
                ],
                compiler_params=pltpu.CompilerParams(collective_id=1 + s, has_side_effects=True, vmem_limit_bytes=VMEM),
                cost_estimate=pl.CostEstimate(flops=6 * length * d * w_down.shape[0], transcendentals=length * w_down.shape[0], bytes_accessed=84 * 2**20),
            )(x2, *chips, *others, gain_m, w_gate, w_up, w_down, after)

        got = first_half()
        sums, others = got[: len(ARRAYS)], [*got[len(ARRAYS) :]]
        others += [over(t) for k, t in enumerate(sums) if k >= CROSSING]
        after, ends = sums[-1], []
        for s in range(batch):
            found = [[(k, c - a[0], a) for k, a in enumerate(ARRAYS) if a[0] <= c < a[0] + a[1]] for c in range(s * per, (s + 1) * per)]
            used = sorted({f[0] for part in found for f in part})
            parts = [[(used.index(k), c * half, a[2], a[3]) for k, c, a in part] for part in found]
            *chips, mine = second_half(s, [sums[k] for k in used], [others[k] for k in used], parts, after)
            after = chips[0]
            ends.append((mine, chips, [over(chip) for chip in chips]))
        y = pl.pallas_call(lambda _, o: None, in_specs=[anywhere], out_specs=anywhere, out_shape=jax.ShapeDtypeStruct(x2.shape, low), name="empty")(after)
        y = y.reshape(batch, per, 2, half, d)
        for s, (mine, chips, others) in enumerate(ends):
            at = 0
            for chip, other in zip(chips, others):
                wide = chip.shape[1]
                other, y = lax.optimization_barrier((other, y))
                t = (mine[:, at : at + wide].astype(jnp.float32) + (chip.astype(jnp.float32) + other.astype(jnp.float32))).astype(low)
                for rows, side in ((t, core), (lax.ppermute(t, "tp", SAME_CHIP), 1 - core)):
                    y = lax.dynamic_update_slice(y, rows.reshape(1, per, 1, half, wide), (s, 0, side, 0, at))
                at += wide
        return y.reshape(x.shape)

    tokens, whole, columns, rows_of = P("dp", None, None), P(None), P(None, "tp"), P("tp", None)
    return jax.shard_map(
        step,
        mesh=mesh,
        in_specs=(tokens, whole, columns, columns, columns, rows_of, whole, columns, columns, rows_of),
        out_specs=tokens,
        check_vma=False,
    )
```

```python
import functools

import jax
import jax.numpy as jnp
import numpy as np
from jax import lax
from jax.experimental import pallas as pl
from jax.experimental.pallas import tpu as pltpu
from jax.sharding import PartitionSpec as P


HEAD = 128
THETA = 10000
LOG2E = 1.4426950408889634
SAME_CHIP = [(0, 1), (1, 0), (2, 3), (3, 2)]
OTHER_CHIP = [(0, 2), (2, 0), (1, 3), (3, 1)]
FINE = 16
ARRAYS = ((0, 3, 0, 4), (3, 1, 0, 4), (4, 2, 0, 4), (6, 2, 0, 4))
CROSSING = 1
LAST = (1536, 1536, 640, 384)
CHUNK = 256
PIECE = 1024
VMEM = 63 * 2**20


def _dot(a, b, ca=1, cb=0):
    return lax.dot_general(a, b, (((ca,), (cb,)), ((), ())), preferred_element_type=jnp.float32)


def rotary(rows):
    half = HEAD // 2
    place = np.concatenate([np.arange(0, rows, FINE), np.arange(FINE)])
    angle = place[:, None] * float(THETA) ** (-np.arange(half) / half)
    return np.stack([np.tile(f(angle), 2) for f in (np.cos, np.sin)]).astype(np.float32)


def _turned(t, cos, sin):
    t = t.astype(jnp.float32)
    return (t * cos + pltpu.roll(t, HEAD // 2, 1) * sin).astype(jnp.bfloat16)


def _normed(parts, gains):
    wide = [p.astype(jnp.float32) for p in parts]
    total = sum(jnp.sum(w * w, -1, keepdims=True) for w in wide)
    scale = lax.rsqrt(total * (1 / sum(w.shape[1] for w in wide)) + 1e-6)
    return [(w * scale * g).astype(jnp.bfloat16) for w, g in zip(wide, gains)]


def _places():
    me = lax.axis_index("tp")
    core = lax.rem(me, 2)
    return core, me + 1 - 2 * core


def _greet(peer):
    pl.semaphore_signal(pltpu.get_barrier_semaphore(), inc=1, device_id={"tp": peer}, device_id_type=pl.DeviceIdType.MESH)


def _to_core(peer, src, dst, send, recv):
    return pltpu.make_async_remote_copy(
        src_ref=src, dst_ref=dst, send_sem=send, recv_sem=recv, device_id={"tp": peer}, device_id_type=pl.DeviceIdType.MESH
    )


def _sum_on_chip(peer, term, out_refs, send_s, recv_s, own_s, sum_s, send_sem, recv_sem, out_sem):
    n, rows = send_s.shape[0], send_s.shape[1]

    def over(i):
        return _to_core(peer, send_s.at[i], recv_s.at[i], send_sem.at[i], recv_sem.at[i])

    def out(i):
        copies, first = [], 0
        for k, ref in enumerate(out_refs):
            last = first + ref.shape[1]
            low, high = max(first, i * PIECE), min(last, (i + 1) * PIECE)
            if low < high:
                here = sum_s.at[i, :, pl.ds(low - i * PIECE, high - low)]
                copies.append(pltpu.make_async_copy(here, ref.at[:, pl.ds(low - first, high - low)], out_sem.at[i, k]))
            first = last
        return copies

    def finish(i):
        over(i).wait_recv()
        sum_s[i] = (own_s[lax.rem(i, 2)] + recv_s[i].astype(jnp.float32)).astype(jnp.bfloat16)

    def piece(i, _):
        t = term(i)
        send_s[i] = t[:rows].astype(jnp.bfloat16)
        own_s[lax.rem(i, 2)] = t[rows:]
        over(i).start()

        @pl.when(i > 0)
        def _():
            finish(i - 1)

    lax.fori_loop(0, n, piece, None)
    for i in range(n):
        if i == n - 1:
            finish(i)
        for c in out(i):
            c.start()
    for i in range(n):
        over(i).wait_send()
        for c in out(i):
            c.wait()


def _first(x_ref, gain_ref, turn_ref, wq_ref, wk_ref, wv_ref, wo_ref, *rest):
    chip_refs, other_refs, rest = rest[: len(ARRAYS)], rest[len(ARRAYS) : len(ARRAYS) + CROSSING], rest[len(ARRAYS) + CROSSING :]
    (x_s, a_s, w_s, wo_s, qkv_s, keys_s, seen_s, turn_s, send_s, recv_s, own_s, sum_s, gain_s, angle_s,
     small_sem, x_sem, w_sem, wo_sem, send_sem, recv_sem, out_sem, x_send_sem, x_recv_sem) = rest
    rows, d = a_s.shape
    half, width, n, chunks = rows // 2, w_s.shape[2], wo_s.shape[0], sum_s.shape[0] // wo_s.shape[0]
    groups = wk_ref.shape[1] // HEAD
    core, peer = _places()
    across = lax.rem(lax.axis_index("tp") + 2, 4)
    _greet(peer)
    _greet(across)

    def fetch(w, to, sem):
        for r in range(0, d, d // 4):
            pltpu.make_async_copy(w.at[pl.ds(r, d // 4), :], to.at[pl.ds(r, d // 4), :], sem).start()


    def x_copy(c):
        return pltpu.make_async_copy(x_ref.at[pl.ds(pl.multiple_of(c * rows, rows), rows), :], x_s.at[lax.rem(c, 2)], x_sem.at[lax.rem(c, 2)])

    def x_part(i):
        here = pl.ds(pl.multiple_of(i * (rows // 4), rows // 4), rows // 4)
        return pltpu.make_async_copy(x_ref.at[here, :], x_s.at[0, here, :], x_sem.at[2 + i])

    def wo_copy(i):
        return pltpu.make_async_copy(wo_ref.at[:, pl.ds(pl.multiple_of(i * PIECE, PIECE), PIECE)], wo_s.at[i], wo_sem.at[i])

    small = [pltpu.make_async_copy(r, t, small_sem.at[i]) for i, (r, t) in enumerate(((gain_ref, gain_s), (turn_ref, angle_s)))]
    for i in range(4):
        x_part(i).start()
    for c in small:
        c.start()
    for i, w in enumerate((wk_ref, wv_ref)):
        fetch(w, w_s.at[0, :, pl.ds(i * width // 2, width // 2)], w_sem.at[0])

    step = 32
    e = HEAD**-0.5 * LOG2E
    hidden = lax.broadcasted_iota(jnp.int32, (rows, rows), 0) > lax.broadcasted_iota(jnp.int32, (rows, rows), 1)

    def over(c, i):
        slot = lax.rem(c, 2) * n + i
        return _to_core(peer, send_s.at[slot], recv_s.at[slot], send_sem.at[slot], recv_sem.at[slot])

    def place_in(array, ref, c, i):
        first, _, column, _ = ARRAYS[array]
        return ref.at[pl.ds(pl.multiple_of((c - first) * half, half), half), pl.ds(pl.multiple_of((i - column) * PIECE, PIECE), PIECE)]

    def cross(array, c, i):
        k = c * n + i
        return _to_core(across, sum_s.at[k], place_in(array, other_refs[array], c, i), x_send_sem.at[k], x_recv_sem.at[k])

    def out(array, c, i):
        return pltpu.make_async_copy(sum_s.at[c * n + i], place_in(array, chip_refs[array], c, i), out_sem.at[c * n + i])

    def finish(c, i):
        over(c, i).wait_recv()
        sum_s[c * n + i] = (own_s[i] + recv_s[lax.rem(c, 2) * n + i].astype(jnp.float32)).astype(jnp.bfloat16)
        for array, (first, count, column, pieces) in enumerate(ARRAYS[:CROSSING]):
            inside = (c >= first) & (c < first + count) & (i >= column) & (i < column + pieces)
            pl.when(inside)(lambda array=array: cross(array, c, i).start())

    def close(c):
        lax.fori_loop(jnp.where(c == 0, n - 1, n - 2), n, lambda i, _: finish(c, i), None)
        for i in range(n):
            over(c, i).wait_send()
        for array, (first, count, column, pieces) in enumerate(ARRAYS):

            @pl.when((c >= first) & (c < first + count))
            def _():
                for i in range(column, column + pieces):
                    out(array, c, i).start()

    def norm(slot, at):
        here = pl.ds(pl.multiple_of(at, step), step)
        a_s[here, :] = _normed([x_s[slot, here, :]], [gain])[0]

    small[0].wait()
    gain = gain_s[...].astype(jnp.float32).reshape(1, d)
    for i in range(w_s.shape[0] - 1):
        fetch(wq_ref.at[:, pl.ds(i * width, width)], w_s.at[i + 1], w_sem.at[i + 1])

    def early(i, _):
        x_part(i).wait()
        lax.fori_loop(0, rows // 4 // step, lambda j, _: norm(0, i * (rows // 4) + j * step), None)

    lax.fori_loop(0, 4, early, None)
    small[1].wait()
    sign = jnp.where(lax.broadcasted_iota(jnp.int32, (1, HEAD), 1) < HEAD // 2, -1.0, 1.0)
    coarse = angle_s.shape[1] - FINE
    cos, sin = angle_s[0, coarse:, :], angle_s[1, coarse:, :]
    for i in range(coarse):
        c, s = angle_s[0, i : i + 1, :], angle_s[1, i : i + 1, :]
        turn_s[0, i * FINE : (i + 1) * FINE, :] = cos * c - sin * s
        turn_s[1, i * FINE : (i + 1) * FINE, :] = (sin * c + cos * s) * sign

    def chunk(c, _):
        late = lax.rem(c, 2)
        place = pl.multiple_of(late * rows, rows)

        @pl.when((c > 0) & (c + 1 < chunks))
        def _():
            x_copy(c + 1).start()

        def project(i, _):
            @pl.when(c == 0)
            def _():
                pltpu.make_async_copy(wq_ref.at[:, pl.ds(0, width)], w_s.at[i], w_sem.at[i]).wait()

            qkv_s[i] = _dot(a_s[...], w_s[i]).astype(jnp.bfloat16)

            @pl.when((i == 0) & (c == 0))
            def _():
                wo_copy(0).start()
                x_copy(1).start()

            @pl.when((i == 1) & (c == 0))
            def _():
                for k in range(1, n):
                    wo_copy(k).start()

        lax.fori_loop(0, w_s.shape[0], project, None)

        @pl.when(c == 0)
        def _():
            pl.semaphore_wait(pltpu.get_barrier_semaphore(), 2)

        pl.when(c > 0)(lambda: close(c - 1))
        new = pl.ds(place, rows)
        for g in range(groups):
            keys_s[new, g * HEAD : (g + 1) * HEAD] = _turned(qkv_s[0, :, g * HEAD : (g + 1) * HEAD], turn_s[0, new, :], turn_s[1, new, :])
        keys_s[new, groups * HEAD :] = qkv_s[0, :, groups * HEAD :]

        def attend(g, _, before):
            total = before + rows
            k = keys_s[:total, pl.ds(pl.multiple_of(g * HEAD, HEAD), HEAD)]
            v = keys_s[:total, pl.ds(pl.multiple_of((g + groups) * HEAD, HEAD), HEAD)]
            values = jnp.concatenate([v.T, jnp.ones((8, total), jnp.bfloat16)], axis=0)
            scores = []
            for h in range(4):
                q = _turned(qkv_s[1 + g, :, h * HEAD : (h + 1) * HEAD], turn_s[0, before:total, :], turn_s[1, before:total, :])
                scores.append(_dot(k, q, 1, 1))
            found = []
            for s in scores:
                last = jnp.where(hidden, -1e30, s[before:])
                s = jnp.concatenate([s[:before], last], axis=0) if before else last
                found.append(jnp.exp2((s - s.max(axis=0, keepdims=True)) * e).astype(jnp.bfloat16))
            for h, p in enumerate(found):
                mix = _dot(values, p)
                got = (mix[:HEAD] * (1 / mix[HEAD : HEAD + 1])).T.astype(jnp.bfloat16)
                for part in range(2):
                    to = pl.ds(pl.multiple_of(jnp.where(core == part, half, 0), half), half)
                    seen_s[to, pl.ds(pl.multiple_of((g * 4 + h) * HEAD, HEAD), HEAD)] = got[part * half : (part + 1) * half]

        @pl.when(late == 0)
        def _():
            for g in range(groups):
                attend(g, None, before=0)

        pl.when(late == 1)(lambda: lax.fori_loop(0, groups, functools.partial(attend, before=rows), None))
        pl.when(c + 1 < chunks)(lambda: x_copy(c + 1).wait())

        def piece(i, _):
            @pl.when(c == 0)
            def _():
                wo_copy(i).wait()

            for j in range(rows // n // step):
                norm(1 - late, (i * (rows // n // step) + j) * step)
            t = _dot(seen_s[...], wo_s[i])
            send_s[late * n + i] = t[:half].astype(jnp.bfloat16)
            own_s[i] = t[half:]
            over(c, i).start()
            pl.when(jnp.where(c == 0, i != 1, i > 1))(lambda: finish(c, jnp.where(c == 0, jnp.maximum(i - 1, 0), i - 2)))

        lax.fori_loop(0, n, piece, None)

    lax.fori_loop(0, chunks, chunk, None)
    close(chunks - 1)
    for array, (first, count, column, pieces) in enumerate(ARRAYS):

        def done(k, _):
            c, i = first + lax.div(k, pieces), column + lax.rem(k, pieces)
            out(array, c, i).wait()
            if array < CROSSING:
                cross(array, c, i).wait_send()
                cross(array, c, i).wait_recv()

        lax.fori_loop(0, count * pieces, done, None)


def _second(x_ref, *refs, parts, first, pieces):
    m = 1 + max(p[0] for part in parts for p in part)
    chips, others, (gain_ref, wg_ref, wu_ref, wd_ref, _), rest = refs[:m], refs[m : 2 * m], refs[2 * m : 2 * m + 5], refs[2 * m + 5 :]
    outs, mine_ref, (in_s, b_s, w_s, hidden_s, wd_s, send_s, recv_s, own_s, sum_s) = rest[:pieces], rest[pieces], rest[pieces + 1 : -9]
    in_sem, mine_sem, b_send_sem, b_recv_sem, w_sem, wd_sem, send_sem, recv_sem, out_sem = rest[-9:]
    rows, d = b_s.shape
    half, wide, n = rows // 2, w_s.shape[2] // 2, send_s.shape[0]
    blocks = wg_ref.shape[1] // wide
    core, peer = _places()
    _greet(peer)

    def weight_copies(i):
        at = pl.ds(pl.multiple_of(i * wide, HEAD), wide)
        slot = lax.rem(i, 2)
        return [pltpu.make_async_copy(w.at[:, at], w_s.at[slot, :, pl.ds(m * wide, wide)], w_sem.at[m, slot]) for m, w in enumerate((wg_ref, wu_ref))]

    def down_copy(i):
        slot = lax.rem(i, 2)
        return pltpu.make_async_copy(wd_ref.at[:, pl.ds(pl.multiple_of(i * PIECE, PIECE), PIECE)], wd_s.at[slot], wd_sem.at[slot])

    load = half // 4
    count = half // len(parts)

    def inputs(i):
        here = pl.ds(pl.multiple_of(i * load, load), load)
        return [pltpu.make_async_copy(x_ref.at[pl.ds(0, load), :], in_s.at[m, here, :], in_sem.at[m, i]) for m in range(3)]

    def fetch(i):
        part, at = divmod(i * load, count)
        here = pl.ds(i * load, load)
        x = x_ref.at[pl.ds(pl.multiple_of(first + 2 * count * part + core * count + at, load), load), :]
        pltpu.make_async_copy(x, in_s.at[0, here, :], in_sem.at[0, i]).start()
        for array, row, column, pieces in parts[part]:
            for m, given in ((1, chips), (2, others)):
                to = in_s.at[m, here, pl.ds(column * PIECE, pieces * PIECE)]
                pltpu.make_async_copy(given[array].at[pl.ds(row + at, load), :], to, in_sem.at[m, i]).start()

    def b_over(i):
        at = pl.multiple_of(i * load, load)
        return _to_core(peer, b_s.at[pl.ds(half + at, load), :], b_s.at[pl.ds(at, load), :], b_send_sem.at[i], b_recv_sem.at[i])

    for i in range(4):
        fetch(i)
    for i in range(2):
        for c in weight_copies(i):
            c.start()

    step = 16
    gain = gain_ref[...].astype(jnp.float32).reshape(1, d)
    pl.semaphore_wait(pltpu.get_barrier_semaphore(), 1)

    def adds(i, _):
        for c in inputs(i):
            c.wait()

        def add(j, _):
            here = pl.ds(pl.multiple_of(i * load + j * step, step), step)
            x, a, b = (in_s[m, here, :].astype(jnp.float32) for m in range(3))
            h = (x + (a + b)).astype(jnp.bfloat16)
            in_s[0, here, :] = h
            b_s[pl.ds(pl.multiple_of(half + i * load + j * step, step), step), :] = _normed([h], [gain])[0]

        lax.fori_loop(0, load // step, add, None)
        b_over(i).start()

    lax.fori_loop(0, 4, adds, None)
    kept = pltpu.make_async_copy(in_s.at[0], mine_ref, mine_sem)
    kept.start()
    for i in range(2):
        down_copy(i).start()
    for i in range(4):
        b_over(i).wait_recv()

    def block(i, _):
        slot = lax.rem(i, 2)
        for c in weight_copies(i):
            c.wait()
        both = _dot(b_s[...], w_s[slot])
        hidden_s[:, pl.ds(pl.multiple_of(i * wide, HEAD), wide)] = (jax.nn.silu(both[:, :wide]) * both[:, wide:]).astype(jnp.bfloat16)

        @pl.when(i + 2 < blocks)
        def _():
            for c in weight_copies(i + 2):
                c.start()

    lax.fori_loop(0, blocks, block, None)

    def term(i):
        down_copy(i).wait()
        t = _dot(hidden_s[...], wd_s[lax.rem(i, 2)])

        @pl.when(i + 2 < n)
        def _():
            down_copy(i + 2).start()

        return t

    _sum_on_chip(peer, term, outs, send_s, recv_s, own_s, sum_s, send_sem, recv_sem, out_sem)
    for i in range(4):
        b_over(i).wait_send()
    kept.wait()


def solution(mesh):
    def step(x, gain_a, wq, wk, wv, wo, gain_m, w_gate, w_up, w_down):
        batch, length, d = x.shape
        n, low, half = d // PIECE, jnp.bfloat16, CHUNK // 2
        chunks, per = batch * length // CHUNK, length // CHUNK
        core = lax.rem(lax.axis_index("tp"), 2)
        turns = rotary(length)
        x2 = x.reshape(batch * length, d)
        dma, anywhere, inside = pltpu.SemaphoreType.DMA, pl.BlockSpec(memory_space=pl.ANY), pl.BlockSpec(memory_space=pltpu.VMEM)
        array = lambda *shape: jax.ShapeDtypeStruct(shape, low)

        def over(t):
            return lax.ppermute(t, "tp", OTHER_CHIP)

        def first_half():
            width, both = 512, 2 * wk.shape[1]
            count = wq.shape[1] // width + 1
            sums = [array(chunks * half, pieces * PIECE) for _, chunks, _, pieces in ARRAYS]
            return pl.pallas_call(
                _first,
                in_specs=[anywhere] * 7,
                out_specs=[anywhere] * (len(ARRAYS) + CROSSING),
                out_shape=[*sums, *sums[:CROSSING]],
                scratch_shapes=[
                    pltpu.VMEM((2, CHUNK, d), low), pltpu.VMEM((CHUNK, d), low), pltpu.VMEM((count, d, width), low),
                    pltpu.VMEM((n, wo.shape[0], PIECE), low), pltpu.VMEM((count, CHUNK, width), low), pltpu.VMEM((length, both), low),
                    pltpu.VMEM((CHUNK, wo.shape[0]), low), pltpu.VMEM((2, length, HEAD), jnp.float32),
                    pltpu.VMEM((2 * n, half, PIECE), low), pltpu.VMEM((2 * n, half, PIECE), low), pltpu.VMEM((n, half, PIECE), jnp.float32),
                    pltpu.VMEM((chunks * n, half, PIECE), low), pltpu.VMEM((d,), low), pltpu.VMEM(turns.shape, jnp.float32),
                    dma((2,)), dma((6,)), dma((count,)), dma((n,)), dma((2 * n,)), dma((2 * n,)), dma((chunks * n,)), dma((chunks * n,)), dma((chunks * n,)),
                ],
                compiler_params=pltpu.CompilerParams(collective_id=0, has_side_effects=True, vmem_limit_bytes=VMEM),
                cost_estimate=pl.CostEstimate(flops=2 * batch * length * d * (2560 + 256), transcendentals=8 * batch * length * length, bytes_accessed=60 * 2**20),
                name="attention",
            )(x2, gain_a, turns, wq, wk, wv, wo)

        def second_half(s, chips, others, parts, after):
            wide, widths, half = 640, LAST if s == batch - 1 else (d,), length // 2
            pieces = len(widths)
            return pl.pallas_call(
                functools.partial(_second, parts=parts, first=s * length, pieces=pieces),
                in_specs=[*[anywhere] * (1 + 2 * len(chips)), inside, *[anywhere] * 4],
                out_specs=[anywhere] * (pieces + 1),
                out_shape=[*(array(half, w) for w in widths), array(half, d)],
                scratch_shapes=[
                    pltpu.VMEM((3, half, d), low), pltpu.VMEM((length, d), low), pltpu.VMEM((2, d, 2 * wide), low),
                    pltpu.VMEM((length, w_down.shape[0]), low), pltpu.VMEM((2, w_down.shape[0], PIECE), low),
                    pltpu.VMEM((n, half, PIECE), low), pltpu.VMEM((n, half, PIECE), low), pltpu.VMEM((2, half, PIECE), jnp.float32), pltpu.VMEM((n, half, PIECE), low),
                    dma((3, 4)), dma, dma((4,)), dma((4,)), dma((2, 2)), dma((2,)), dma((n,)), dma((n,)), dma((n, pieces)),
                ],
                compiler_params=pltpu.CompilerParams(collective_id=1 + s, has_side_effects=True, vmem_limit_bytes=VMEM),
                cost_estimate=pl.CostEstimate(flops=6 * length * d * w_down.shape[0], transcendentals=length * w_down.shape[0], bytes_accessed=84 * 2**20),
            )(x2, *chips, *others, gain_m, w_gate, w_up, w_down, after)

        got = first_half()
        sums, others = got[: len(ARRAYS)], [*got[len(ARRAYS) :]]
        others += [over(t) for k, t in enumerate(sums) if k >= CROSSING]
        after, ends = sums[-1], []
        for s in range(batch):
            found = [[(k, c - a[0], a) for k, a in enumerate(ARRAYS) if a[0] <= c < a[0] + a[1]] for c in range(s * per, (s + 1) * per)]
            used = sorted({f[0] for part in found for f in part})
            parts = [[(used.index(k), c * half, a[2], a[3]) for k, c, a in part] for part in found]
            *chips, mine = second_half(s, [sums[k] for k in used], [others[k] for k in used], parts, after)
            after = chips[0]
            ends.append((mine, chips, [over(chip) for chip in chips]))
        y = pl.pallas_call(lambda _, o: None, in_specs=[anywhere], out_specs=anywhere, out_shape=jax.ShapeDtypeStruct(x2.shape, low), name="empty")(after)
        y = y.reshape(batch, per, 2, half, d)
        for s, (mine, chips, others) in enumerate(ends):
            at = 0
            for chip, other in zip(chips, others):
                wide = chip.shape[1]
                other, y = lax.optimization_barrier((other, y))
                t = (mine[:, at : at + wide].astype(jnp.float32) + (chip.astype(jnp.float32) + other.astype(jnp.float32))).astype(low)
                for rows, side in ((t, core), (lax.ppermute(t, "tp", SAME_CHIP), 1 - core)):
                    y = lax.dynamic_update_slice(y, rows.reshape(1, per, 1, half, wide), (s, 0, side, 0, at))
                at += wide
        return y.reshape(x.shape)

    tokens, whole, columns, rows_of = P("dp", None, None), P(None), P(None, "tp"), P("tp", None)
    return jax.shard_map(
        step,
        mesh=mesh,
        in_specs=(tokens, whole, columns, columns, columns, rows_of, whole, columns, columns, rows_of),
        out_specs=tokens,
        check_vma=False,
    )
```
